32 devices in a mesh: head: 4 (over y, x), blk: 8 (over z, core).
Axes of the slice: x: 2, y: 2, z: 4, core: 2. Of those that a mesh axis runs over, the one named last changes fastest.
Arguments:
- hidden_in: bfloat16 [2048, 4096], P(('blk', 'head')), may hold values from -6 to 6
- queries: bfloat16 [2048, 2048], P(('blk', 'head')), may hold values from -26 to 26
- key_states: bfloat16 [2048, 1024], P(('blk', 'head')), may hold values from -5 to 5
- value_states: bfloat16 [2048, 1024], P(('blk', 'head')), may hold values from -6 to 6
- out_weight: bfloat16 [2048, 4096], P('head'), may hold values from -0.125 to 0.125
- norm_gain: float32 [4096], replicated, may hold values from 0.1 to 1.9
- gate_weight: bfloat16 [4096, 7168], P(None, 'head'), may hold values from -0.09375 to 0.09375
- up_weight: bfloat16 [4096, 7168], P(None, 'head'), may hold values from -0.09375 to 0.09375
- down_weight: bfloat16 [7168, 4096], P('head'), may hold values from -0.0625 to 0.0625
Outputs:
- layer_out: bfloat16 [2048, 4096], P(('blk', 'head'))
The draws below stay inside these ranges and needn't reach their ends.
All inputs are finite; a program needn't handle non-finite values.
Results may differ from the reference program's by a relative error of at most 0.018.
Values may be sent and summed in bfloat16 or wider, within the bound.
A program may use at most 192 MiB of HBM per device.

```python
import jax
import jax.numpy as jnp
from jax import lax

D = 4096
HEADS = 16
KV_HEADS = 8
HEAD_DIM = 128
FF = 7168
TOK_BLK = 256
SEQ = 2048


def paired_draw(seed_key):
    anchor = jax.random.fold_in(seed_key, 7)
    stream_keys = jax.random.fold_in(anchor, 1)
    stream_query = jax.random.fold_in(anchor, 2)
    key_width = KV_HEADS * HEAD_DIM
    query_width = HEADS * HEAD_DIM
    key_drawn = jnp.clip(jax.random.normal(stream_keys, (SEQ, key_width), jnp.float32), -5.0, 5.0)
    query_drawn = jnp.clip(2.5 * jax.random.normal(stream_query, (SEQ, query_width), jnp.float32), -15.0, 15.0)
    return (query_drawn, key_drawn)


def draw_queries(key, part):
    return paired_draw(key)[0].astype(jnp.bfloat16)


def draw_key_states(key, part):
    return paired_draw(key)[1].astype(jnp.bfloat16)


def levels(rng, extent, pieces, least, top_value):
    loudness = 1.0
    for axis_at, blocks in pieces:
        heights = jax.random.uniform(jax.random.fold_in(jax.random.fold_in(rng, 6), axis_at), (blocks,), jnp.float32, least / len(pieces), top_value / len(pieces))
        loudness = loudness * jnp.repeat(jnp.exp(heights), extent[axis_at] // blocks).reshape((-1,) + (1,) * (len(extent) - 1 - axis_at))
    return loudness


def normal_values(key, extent, width, reach, pieces=(), held_as=jnp.bfloat16):
    drawn = jax.random.normal(key, extent, jnp.float32) * width
    if len(pieces) > 0:
        drawn = levels(key, extent, pieces, -0.22, 0.18) * drawn
    return jnp.clip(drawn, min=-reach, max=reach).astype(held_as)


def setup_inputs(seed: int = 0) -> dict:
    splits = jax.random.split(jax.random.key(seed), 10)
    return {
        "hidden_in": normal_values(splits[0], (SEQ, D), 1.0, 6.0, ((0, 32),)),
        "queries": draw_queries(jax.random.fold_in(splits[9], 71), 0),
        "key_states": draw_key_states(jax.random.fold_in(splits[9], 71), 0),
        "value_states": normal_values(splits[3], (SEQ, KV_HEADS * HEAD_DIM), 1.0, 6.0, ((0, 32),)),
        "out_weight": normal_values(splits[4], (HEADS * HEAD_DIM, D), (HEADS * HEAD_DIM) ** -0.5, 0.125, ((0, 4),)),
        "norm_gain": jnp.clip(1.0 + 0.18 * jax.random.normal(splits[5], (D,), jnp.float32), 0.1, 1.9),
        "gate_weight": normal_values(splits[6], (D, FF), D ** -0.5, 0.09375, ((1, 4),)),
        "up_weight": normal_values(splits[7], (D, FF), D ** -0.5, 0.09375, ((1, 4),)),
        "down_weight": normal_values(splits[8], (FF, D), FF ** -0.5, 0.0625, ((0, 4),)),
    }


def attend_group(query_group, key_group, value_group):
    score_scale = HEAD_DIM ** (-0.5)
    positions = jnp.arange(SEQ, dtype=jnp.int32)

    def one_block(block_index):
        first_row = block_index * TOK_BLK
        query_block = lax.dynamic_slice_in_dim(query_group, first_row, TOK_BLK, 1)
        scores = jnp.einsum('rqd,kd->rqk', query_block, key_group) * score_scale
        query_pos = first_row + jnp.arange(TOK_BLK, dtype=jnp.int32)
        visible = positions[None, :] <= query_pos[:, None]
        row_peak = lax.optimization_barrier(jnp.max(jnp.where(visible, scores, -jnp.inf), axis=-1))
        exp_scores = jnp.where(visible, jnp.exp(scores - row_peak[..., None]), 0.0)
        row_total = lax.optimization_barrier(jnp.sum(exp_scores, axis=-1))
        rounded = lax.optimization_barrier(exp_scores.astype(jnp.bfloat16)).astype(jnp.float32)
        numerator = jnp.einsum('rqk,kd->rqd', rounded, value_group)
        return (numerator / row_total[..., None]).astype(jnp.bfloat16)
    return lax.map(one_block, jnp.arange(SEQ // TOK_BLK, dtype=jnp.int32))

def attend_tuple(groups):
    return attend_group(groups[0], groups[1], groups[2])

def reference(hidden_in, queries, key_states, value_states, out_weight, norm_gain, gate_weight, up_weight, down_weight):
    group_ratio = HEADS // KV_HEADS
    query_all = queries.astype(jnp.float32).reshape(SEQ, KV_HEADS, group_ratio, HEAD_DIM).transpose(1, 2, 0, 3)
    key_all = key_states.astype(jnp.float32).reshape(SEQ, KV_HEADS, HEAD_DIM).transpose(1, 0, 2)
    value_all = value_states.astype(jnp.float32).reshape(SEQ, KV_HEADS, HEAD_DIM).transpose(1, 0, 2)
    attended = lax.map(attend_tuple, (query_all, key_all, value_all))
    attended = attended.transpose(1, 3, 0, 2, 4).reshape(SEQ, HEADS * HEAD_DIM)
    projected = jnp.dot(attended, out_weight, preferred_element_type=jnp.float32)
    residual = (hidden_in.astype(jnp.float32) + projected).astype(jnp.bfloat16)
    widened = residual.astype(jnp.float32)
    mean_square = lax.optimization_barrier(jnp.mean(widened * widened, axis=-1, keepdims=True))
    normed = (widened * lax.rsqrt(mean_square + 1e-05) * norm_gain.astype(jnp.float32)).astype(jnp.bfloat16)
    gate_part = jnp.dot(normed, gate_weight, preferred_element_type=jnp.float32)
    up_part = jnp.dot(normed, up_weight, preferred_element_type=jnp.float32)
    inner_act = (jax.nn.silu(gate_part) * up_part).astype(jnp.bfloat16)
    mlp_out = jnp.dot(inner_act, down_weight, preferred_element_type=jnp.float32)
    return (residual.astype(jnp.float32) + mlp_out).astype(jnp.bfloat16)
```

```python
import functools

import jax
import jax.numpy as jnp
from jax import lax
from jax.experimental import pallas as pl
from jax.experimental.pallas import tpu as pltpu
from jax.sharding import PartitionSpec as P

HEADS = 16
KV_HEADS = 8
HEAD_DIM = 128
CHUNKS = 4
AHEAD = 2
SUBS = 4
LEAD = 4
RCHUNKS = 8
LOG2E = 1.4426950408889634
MESH = pl.DeviceIdType.MESH
BF = jnp.bfloat16
F32 = jnp.float32


def tile_of(n, most=256):
    t = most
    while n % t:
        t -= 128
    return t


def remote(src, dst, send, recv, axis, index):
    return pltpu.make_async_remote_copy(
        src_ref=src, dst_ref=dst, send_sem=send, recv_sem=recv,
        device_id={axis: index}, device_id_type=MESH,
    )


def general_kernel(
    H, B,
    hid, q_in, k_in, v_in, gain, wo_h, wg_h, wu_h, wd_h,
    out,
    wo, wg, wu, wd, qb, kv, att, part, rs, gath, accg, accu, inner,
    w_sem, loc_sem, a_s, a_r, z_s, z_r, d_s, d_r, rs_s, rs_r, ag_s, ag_r, r2_s, r2_r,
):
    h = lax.axis_index("head")
    b = lax.axis_index("blk")
    J = B // 2
    j = b // 2
    c = b % 2
    partner = b + 1 - 2 * c
    T = hid.shape[0]
    D = hid.shape[1]
    R = T * H
    QW = qb.shape[1]
    KW = kv.shape[3]
    nh = QW // HEAD_DIM
    ratio = HEADS // KV_HEADS
    CW = D // CHUNKS
    FW = wg.shape[1]

    wcopies = [pltpu.make_async_copy(wo_h, wo, w_sem.at[0])]
    for i in range(CHUNKS):
        rows = pl.ds(i * CW, CW)
        wcopies.append(pltpu.make_async_copy(wg_h.at[rows], wg.at[rows], w_sem.at[1 + 2 * i]))
        wcopies.append(pltpu.make_async_copy(wu_h.at[rows], wu.at[rows], w_sem.at[2 + 2 * i]))
    wcopies.append(pltpu.make_async_copy(wd_h, wd, w_sem.at[1 + 2 * CHUNKS]))
    barrier = pltpu.get_barrier_semaphore()
    for d in range(1, H):
        pl.semaphore_signal(barrier, inc=1, device_id={"head": lax.rem(h + d, H)}, device_id_type=MESH)

    @pl.when(j > 0)
    def _():
        pl.semaphore_signal(barrier, inc=1, device_id={"blk": lax.rem(b + B - 2, B)}, device_id_type=MESH)

    @pl.when(j < J - 1)
    def _():
        pl.semaphore_signal(barrier, inc=1, device_id={"blk": lax.rem(b + 2, B)}, device_id_type=MESH)

    pl.semaphore_signal(barrier, inc=1, device_id={"blk": partner}, device_id_type=MESH)
    pl.semaphore_wait(barrier, H + jnp.minimum(j, 1) + jnp.minimum(J - 1 - j, 1))

    my_rows = pl.ds(pl.multiple_of(h * T, T), T)

    def cols(p, w):
        return pl.ds(pl.multiple_of(p * w, w), w)

    a_copies = []
    for t, (src, dst, w) in enumerate(
        ((k_in, kv.at[b, 0], KW), (v_in, kv.at[b, 1], KW), (q_in, qb, QW))
    ):
        for d in range(1, H):
            p = lax.rem(h + d, H)
            cp = remote(
                src.at[:, cols(p, w)], dst.at[my_rows, :],
                a_s.at[d - 1, t], a_r.at[d - 1, t], "head", p,
            )
            cp.start()
            a_copies.append((t, cp))
        lc = pltpu.make_async_copy(src.at[:, cols(h, w)], dst.at[my_rows, :], loc_sem.at[t])
        lc.start()
        a_copies.append((t, lc))

    def wait_in(t):
        for tt, cp in a_copies:
            if tt == t:
                cp.wait()

    def z_copy(slot, t):
        return remote(
            kv.at[slot, t], kv.at[slot, t], z_s.at[slot, t], z_r.at[slot, t],
            "blk", lax.rem(b + 2, B),
        )

    def d_copy(slot, t):
        return remote(
            kv.at[slot, t], kv.at[slot, t], d_s.at[slot, t], d_r.at[slot, t], "blk", partner
        )

    for t in range(2):
        wait_in(t)

        @pl.when(j < J - 1)
        def _():
            z_copy(b, t).start()

        @pl.when(c == 0)
        def _():
            d_copy(b, t).start()

    wait_in(2)
    for w in wcopies:
        w.start()

    mq = lambda n: slice(n * HEAD_DIM, (n + 1) * HEAD_DIM)
    ml = lambda n: slice((nh + n) * HEAD_DIM, (nh + n + 1) * HEAD_DIM)
    scale = HEAD_DIM ** (-0.5)

    def absorb(slot, first):
        for n in range(nh):
            g = n // ratio
            s = lax.dot_general(
                qb[:, mq(n)], kv[slot, 0, :, mq(g)],
                (((1,), (1,)), ((), ())), preferred_element_type=F32,
            ) * scale
            if first:
                qi = lax.broadcasted_iota(jnp.int32, s.shape, 0)
                ki = lax.broadcasted_iota(jnp.int32, s.shape, 1)
                s = jnp.where(ki <= qi, s, -1e30)
            top = jnp.max(s, axis=1, keepdims=True)
            if not first:
                old = accu[:, mq(n)][:, :1]
                top = jnp.maximum(top, old)
            e = jnp.exp(s - top)
            tot = jnp.sum(e, axis=1, keepdims=True)
            pv = jnp.dot(e.astype(BF), kv[slot, 1, :, mq(g)], preferred_element_type=F32)
            if not first:
                f = jnp.exp(old - top)
                tot = tot + accu[:, ml(n)][:, :1] * f
                pv = pv + accg[:, mq(n)] * f
            accu[:, mq(n)] = jnp.broadcast_to(top, (R, HEAD_DIM))
            accu[:, ml(n)] = jnp.broadcast_to(tot, (R, HEAD_DIM))
            accg[:, mq(n)] = pv

    absorb(b, True)

    @pl.when(c == 1)
    def _():
        for t in range(2):
            d_copy(b - 1, t).wait_recv()
        absorb(b - 1, False)

    def chain(s, carry):
        slot = 2 * (j - 1 - s) + c
        other = 2 * (j - 1 - s) + 1 - c
        for t in range(2):
            z_copy(slot, t).wait_recv()

            @pl.when(j < J - 1)
            def _():
                z_copy(slot, t).start()

            d_copy(slot, t).start()
        absorb(slot, False)
        for t in range(2):
            d_copy(other, t).wait_recv()
        absorb(other, False)
        return carry

    lax.fori_loop(0, j, chain, 0)

    for n in range(nh):
        att[:, mq(n)] = (accg[:, mq(n)] / accu[:, ml(n)]).astype(BF)

    square_ring = H == 4
    nx = h + 1 - 2 * (h % 2)
    ny = lax.rem(h + H // 2, H)
    dg = H - 1 - h
    HW = CW // 2

    def rows_of(p):
        return pl.ds(pl.multiple_of(p * T, T), T)

    def halves(i):
        return pl.ds(i * CW, HW), pl.ds(i * CW + HW, HW)

    def scatter(w_ref, x_ref, send, recv):
        copies = {}
        ct = tile_of(CW)
        for i in range(CHUNKS):
            def step(t, carry):
                cs = pl.ds(pl.multiple_of(i * CW + t * ct, ct), ct)
                part[:, cs] = jnp.dot(
                    x_ref[...], w_ref[:, cs], preferred_element_type=F32
                ).astype(BF)
                return carry

            lax.fori_loop(0, CW // ct, step, 0)
            if square_ring:
                ha, hb = halves(i)
                plan = ((1, dg, ha, 0, nx), (1, dg, hb, 1, ny), (0, nx, ha, 2, nx), (0, ny, hb, 3, ny))
            else:
                cs = pl.ds(i * CW, CW)
                plan = [(d - 1, lax.rem(h + d, H), cs, d - 1, lax.rem(h + d, H)) for d in range(1, H)]
            for place, block, cs, sem, to in plan:
                cp = remote(
                    part.at[rows_of(block), cs], rs.at[place, :, cs],
                    send.at[sem, i], recv.at[sem, i], "head", to,
                )
                cp.start()
                copies[sem, i] = cp
        return copies

    def combine(i, copies, send, recv):
        if not square_ring:
            return
        ha, hb = halves(i)
        for cs, sem, to in ((ha, 0, ny), (hb, 1, nx)):
            copies[sem, i].wait_recv()
            blk_rows = rows_of(to)
            part[blk_rows, cs] = (
                part[blk_rows, cs].astype(F32) + rs[1, :, cs].astype(F32)
            ).astype(BF)
            cp = remote(
                part.at[blk_rows, cs], rs.at[2, :, cs],
                send.at[4 + sem, i], recv.at[4 + sem, i], "head", to,
            )
            cp.start()
            copies[4 + sem, i] = cp

    def reduced(i, copies):
        cs = pl.ds(i * CW, CW)
        sems = (2, 3, 4, 5) if square_ring else range(H - 1)
        for sem in sems:
            copies[sem, i].wait_recv()
        total = part[my_rows, cs].astype(F32)
        for place in (0, 2) if square_ring else range(H - 1):
            total = total + rs[place, :, cs].astype(F32)
        return total

    wcopies[0].wait()
    rs_copies = scatter(wo, att, rs_s, rs_r)
    ag_copies = {}

    def spread(rows, cs, sem, i, to):
        cp = remote(
            gath.at[rows, cs], gath.at[rows, cs],
            ag_s.at[sem, i], ag_r.at[sem, i], "head", to,
        )
        cp.start()
        ag_copies[sem, i] = cp

    def spread_own(i):
        for sem, to in enumerate(
            (nx, ny) if square_ring else [lax.rem(h + d, H) for d in range(1, H)]
        ):
            spread(my_rows, pl.ds(i * CW, CW), sem, i, to)

    for i in range(CHUNKS + 1):
        if i < CHUNKS:
            combine(i, rs_copies, rs_s, rs_r)
        if i:
            cs = pl.ds((i - 1) * CW, CW)
            gath[my_rows, cs] = (hid[:, cs].astype(F32) + reduced(i - 1, rs_copies)).astype(BF)
            if i <= AHEAD or not square_ring:
                spread_own(i - 1)

    ft = tile_of(FW)
    square = jnp.zeros((R, 1), F32)
    for i in range(CHUNKS + 1):
        if i < CHUNKS and square_ring:
            ha, hb = halves(i)
            ag_copies[0, i].wait_recv()
            spread(rows_of(nx), ha, 2, i, ny)
            ag_copies[1, i].wait_recv()
            spread(rows_of(ny), hb, 3, i, nx)
            if i + AHEAD < CHUNKS:
                spread_own(i + AHEAD)
        if i == 0:
            continue
        k = i - 1
        cs = pl.ds(k * CW, CW)
        for sem in (2, 3) if square_ring else range(H - 1):
            ag_copies[sem, k].wait_recv()
        wcopies[1 + 2 * k].wait()
        wcopies[2 + 2 * k].wait()
        x = gath[:, cs].astype(F32)
        square = square + jnp.sum(x * x, axis=1, keepdims=True)
        xg = (x * gain[:, cs]).astype(BF)

        def step(t, carry, xg=xg, cs=cs, k=k):
            fs = pl.ds(pl.multiple_of(t * ft, ft), ft)
            g = jnp.dot(xg, wg[cs, fs], preferred_element_type=F32)
            u = jnp.dot(xg, wu[cs, fs], preferred_element_type=F32)
            if k:
                g = g + accg[:, fs]
                u = u + accu[:, fs]
            accg[:, fs] = g
            accu[:, fs] = u
            return carry

        lax.fori_loop(0, FW // ft, step, 0)
    r = lax.rsqrt(square / D + 1e-5)

    def act(t, carry):
        fs = pl.ds(pl.multiple_of(t * ft, ft), ft)
        g = accg[:, fs] * r
        u = accu[:, fs] * r
        inner[:, fs] = (g / (1.0 + jnp.exp(-g)) * u).astype(BF)
        return carry

    lax.fori_loop(0, FW // ft, act, 0)
    for cp in rs_copies.values():
        cp.wait_send()
    wcopies[-1].wait()
    r2_copies = scatter(wd, inner, r2_s, r2_r)
    for i in range(CHUNKS + 1):
        if i < CHUNKS:
            combine(i, r2_copies, r2_s, r2_r)
        if i:
            cs = pl.ds((i - 1) * CW, CW)
            out[:, cs] = (gath[my_rows, cs].astype(F32) + reduced(i - 1, r2_copies)).astype(BF)

    for cp in (*ag_copies.values(), *r2_copies.values()):
        cp.wait_send()
    for t in range(2):
        @pl.when(j < J - 1)
        def _():
            z_copy(b, t).wait_send()

        @pl.when(c == 0)
        def _():
            d_copy(b, t).wait_send()

    def drain(s, carry):
        slot = 2 * (j - 1 - s) + c
        for t in range(2):
            @pl.when(j < J - 1)
            def _():
                z_copy(slot, t).wait_send()

            d_copy(slot, t).wait_send()
        return carry

    lax.fori_loop(0, j, drain, 0)


def square_kernel(
    H, B,
    hid, q_in, k_in, v_in, gain, wo_h, wg_h, wu_h, wd_h,
    out,
    wo, wg, wu, wd, qb, kv, att, attx, hx, sb, rb, part, rs, gath, accg, accu, inner,
    w_sem, a_s, a_r, z_s, z_r, d_s, d_r, x_s, x_r, at_s, at_r, o_s, o_r, ag_s, ag_r, r2_s, r2_r,
):
    h = lax.axis_index("head")
    b = lax.axis_index("blk")
    J = B // 2
    j = b // 2
    c = b % 2
    partner = b + 1 - 2 * c
    T, D = hid.shape
    R = T * H
    G, QR = qb.shape[0], qb.shape[1]
    ratio = QR // R
    QW = att.shape[1]
    GW = QW // G
    FW = wg.shape[1]
    half = D // 2
    DW = D // 4
    SW = DW // SUBS
    CW = D // RCHUNKS

    ex, ey = h % 2, h // 2
    nx = h + 1 - 2 * ex
    ny = lax.rem(h + 2, H)
    dg = H - 1 - h
    pair = (nx, ny)
    across = (ny, nx)
    mine = (ex, ey)

    wcopies = []
    for s in range(2):
        src = wo_h.at[:, pl.ds(pl.multiple_of(s * half + mine[s] * DW, DW), DW)]
        wcopies.append((src, wo.at[s, pl.ds(0, QW)]))
    for i in range(CHUNKS):
        rows = pl.ds(i * (D // CHUNKS), D // CHUNKS)
        wcopies.append((wg_h.at[rows], wg.at[rows]))
        wcopies.append((wu_h.at[rows], wu.at[rows]))
    wcopies.append((wd_h, wd))
    wcopies = [pltpu.make_async_copy(s, d, w_sem.at[n]) for n, (s, d) in enumerate(wcopies)]

    barrier = pltpu.get_barrier_semaphore()
    for d in range(1, H):
        pl.semaphore_signal(barrier, inc=1, device_id={"head": lax.rem(h + d, H)}, device_id_type=MESH)

    @pl.when(j > 0)
    def _():
        pl.semaphore_signal(barrier, inc=1, device_id={"blk": lax.rem(b + B - 2, B)}, device_id_type=MESH)

    @pl.when(j < J - 1)
    def _():
        pl.semaphore_signal(barrier, inc=1, device_id={"blk": lax.rem(b + 2, B)}, device_id_type=MESH)

    pl.semaphore_signal(barrier, inc=1, device_id={"blk": partner}, device_id_type=MESH)
    pl.semaphore_wait(barrier, H + jnp.minimum(j, 1) + jnp.minimum(J - 1 - j, 1))

    def rows_of(p):
        return pl.ds(pl.multiple_of(p * T, T), T)

    my_rows = rows_of(h)

    def head_cols(n):
        return pl.ds(pl.multiple_of(n * HEAD_DIM, HEAD_DIM), HEAD_DIM)

    def q_rows(r, p):
        return pl.ds(pl.multiple_of(r * R + p * T, T), T)

    pieces = []
    for g in range(G):
        pieces.append((k_in, G, g, lambda p, g=g: kv.at[b, g, 0, rows_of(p), :]))
        pieces.append((v_in, G, g, lambda p, g=g: kv.at[b, g, 1, rows_of(p), :]))
    for n in range(G * ratio):
        pieces.append((q_in, G * ratio, n, lambda p, n=n: qb.at[n // ratio, q_rows(n % ratio, p), :]))
    a_copies = []
    for t, (src, per, n, dst) in enumerate(pieces):
        cps = []
        for d, p in enumerate((dg, nx, ny)):
            cp = remote(src.at[:, head_cols(p * per + n)], dst(h), a_s.at[d, t], a_r.at[d, t], "head", p)
            cp.start()
            cps.append(cp)
        a_copies.append(cps)

    x_copies = []
    for s in range(2):
        cs = pl.ds(pl.multiple_of(s * half + (1 - mine[s]) * DW, DW), DW)
        x_copies.append(remote(hid.at[:, cs], hx.at[s], x_s.at[s], x_r.at[s], "head", pair[s]))
    core_cols = pl.ds(pl.multiple_of(c * (DW // 2), DW // 2), DW // 2)
    for s in range(2):
        cs = pl.ds(pl.multiple_of(s * half + (1 - mine[s]) * DW + c * (DW // 2), DW // 2), DW // 2)
        x_copies.append(remote(
            wo_h.at[:, cs], wo.at[s, pl.ds(QW, QW), core_cols],
            x_s.at[2 + s], x_r.at[2 + s], "head", pair[s],
        ))
    for cp in x_copies:
        cp.start()
    share = []
    for s in range(2):
        ref = wo.at[s, pl.ds(QW, QW), core_cols]
        share.append(remote(ref, ref, x_s.at[4 + s], x_r.at[4 + s], "blk", partner))

    for t, (src, per, n, dst) in enumerate(pieces):
        dst(h)[...] = src[:, head_cols(h * per + n)]

    def wait_in(t):
        for cp in a_copies[t]:
            cp.wait_recv()

    def z_copy(slot, g, t):
        ref = kv.at[slot, g, t]
        return remote(ref, ref, z_s.at[slot, g, t], z_r.at[slot, g, t], "blk", lax.rem(b + 2, B))

    def d_copy(slot, g, t):
        ref = kv.at[slot, g, t]
        return remote(ref, ref, d_s.at[slot, g, t], d_r.at[slot, g, t], "blk", partner)

    own = [(g, t) for g in range(G) for t in range(2)]
    for n, (g, t) in enumerate(own):
        wait_in(n)

        @pl.when((j < J - 1) & ((j == 0) | (n < len(own) - 1)))
        def _():
            z_copy(b, g, t).start()

        @pl.when(c == 0)
        def _():
            d_copy(b, g, t).start()

    def pass_on(slot, g, t):
        z_copy(slot, g, t).wait_recv()

        @pl.when(j < J - 1)
        def _():
            z_copy(slot, g, t).start()

        d_copy(slot, g, t).start()

    def arrive(s, g):
        slot = 2 * (j - 1 - s) + c
        other = 2 * (j - 1 - s) + 1 - c
        for t in range(2):
            pass_on(slot, g, t)
        if g == 0:
            @pl.when((s == 0) & (j < J - 1))
            def _():
                z_copy(b, *own[-1]).start()
        for t in range(2):
            d_copy(other, g, t).wait_recv()
        return slot, other

    for n in range(G * ratio):
        wait_in(len(own) + n)
    for w in wcopies:
        w.start()

    factor = HEAD_DIM ** (-0.5) * LOG2E

    def absorb(g, slots, first):
        for r in range(ratio):
            qh = qb[g, r * R:(r + 1) * R, :]
            scores = []
            n = g * ratio + r
            tops = slice(n * HEAD_DIM, (n + 1) * HEAD_DIM)
            sums = slice(2 * n * HEAD_DIM, 2 * (n + 1) * HEAD_DIM)
            for slot in slots:
                sc = lax.dot_general(
                    qh, kv[slot, g, 0], (((1,), (1,)), ((), ())), preferred_element_type=F32,
                )
                if first:
                    qi = lax.broadcasted_iota(jnp.int32, sc.shape, 0)
                    ki = lax.broadcasted_iota(jnp.int32, sc.shape, 1)
                    sc = jnp.where(ki <= qi, sc, -1e30)
                scores.append(sc)
            top = jnp.max(scores[0], axis=1, keepdims=True)
            for sc in scores[1:]:
                top = jnp.maximum(top, jnp.max(sc, axis=1, keepdims=True))
            if not first:
                old = accu[:, tops][:, :1]
                top = jnp.maximum(top, old)
            pv = None
            for sc, slot in zip(scores, slots):
                e = jnp.exp2((sc - top) * factor).astype(BF)
                v = kv[slot, g, 1]
                term = jnp.dot(
                    e, jnp.concatenate([v, jnp.ones_like(v)], axis=1), preferred_element_type=F32
                )
                pv = term if pv is None else pv + term
            if not first:
                pv = pv + accg[:, sums] * jnp.exp2((old - top) * factor)
            accu[:, tops] = jnp.broadcast_to(top, (R, HEAD_DIM))
            accg[:, sums] = pv

    at_copies = []
    for g in range(G):
        absorb(g, (b,), True)

        @pl.when(c == 1)
        def _(g=g):
            for t in range(2):
                d_copy(b - 1, g, t).wait_recv()
            absorb(g, (b - 1,), False)

        def chain(s, carry, g=g):
            absorb(g, arrive(s, g), False)
            return carry

        lax.fori_loop(0, j, chain, 0)
        for r in range(ratio):
            n = g * ratio + r
            pv = accg[:, 2 * n * HEAD_DIM:2 * (n + 1) * HEAD_DIM]
            att[:, n * HEAD_DIM:(n + 1) * HEAD_DIM] = (pv[:, :HEAD_DIM] / pv[:, HEAD_DIM:]).astype(BF)
        cs = pl.ds(g * GW, GW)
        for s in range(2):
            cp = remote(att.at[:, cs], attx.at[s, :, cs], at_s.at[g, s], at_r.at[g, s], "head", pair[s])
            cp.start()
            at_copies.append(cp)

    accs = (accg, accu)
    for s in range(2):
        x_copies[2 + s].wait_recv()
        share[s].start()
    for s in range(2):
        wcopies[s].wait()
        tile = tile_of(DW)

        def own_part(t, carry, s=s):
            cs = pl.ds(pl.multiple_of(t * tile, tile), tile)
            accs[s][:, cs] = jnp.dot(att[...], wo[s, :QW, cs], preferred_element_type=F32)
            return carry

        lax.fori_loop(0, DW // tile, own_part, 0)
    for s in range(2):
        share[s].wait_recv()
    for cp in at_copies:
        cp.wait_recv()

    co = ({"h": nx, "x": h, "y": dg, "d": ny}, {"h": ny, "x": dg, "y": h, "d": nx})
    order = [(s, i) for i in range(SUBS) for s in range(2)]
    o_copies = {}
    for s, i in order:
        cs = pl.ds(i * SW, SW)
        accs[s][:, cs] += jnp.dot(attx[s], wo[s, QW:, i * SW:(i + 1) * SW], preferred_element_type=F32)
        to = across[s]
        away = (to, co[s]["y" if s == 0 else "x"])
        for n, p in enumerate(away):
            sb[s, n * T:(n + 1) * T, i * SW:(i + 1) * SW] = accs[s][rows_of(p), cs].astype(BF)
        cp = remote(sb.at[s, :, cs], rb.at[s, :, cs], o_s.at[s, i], o_r.at[s, i], "head", to)
        cp.start()
        o_copies[s, i] = cp

    def cols_of(s, i, other):
        part_index = 1 - mine[s] if other else mine[s]
        return pl.ds(pl.multiple_of(s * half + part_index * DW + i * SW, SW), SW)

    ag_copies = {}

    def spread(s, i, kind, rows, cs, to):
        ref = gath.at[rows, cs]
        cp = remote(ref, ref, ag_s.at[s, i, kind], ag_r.at[s, i, kind], "head", to)
        cp.start()
        ag_copies[s, i, kind] = cp

    def spread_own(s, i):
        cs = cols_of(s, i, False)
        for n, to in enumerate((nx, ny)):
            spread(s, i, 2 * n, my_rows, cs, to)
            spread(s, i, 2 * n + 1, rows_of(co[s]["h"]), cs, to)

    def relay(s, i):
        ag_copies[s, i, 0].wait_recv()
        spread(s, i, 4, rows_of(nx), cols_of(s, i, s == 0), ny)
        ag_copies[s, i, 3].wait_recv()
        spread(s, i, 5, rows_of(co[s]["y"]), cols_of(s, i, s == 1), nx)

    for s in range(2):
        x_copies[s].wait_recv()
    for k, (s, i) in enumerate(order):
        o_copies[s, i].wait_recv()
        cs = cols_of(s, i, False)
        lc = slice(i * SW, (i + 1) * SW)
        gath[my_rows, cs] = (
            hid[:, cs].astype(F32) + (accs[s][my_rows, lc] + rb[s, :T, lc].astype(F32))
        ).astype(BF)
        cr = rows_of(co[s]["h"])
        gath[cr, cs] = (
            hx[s, :, lc].astype(F32) + (accs[s][cr, lc] + rb[s, T:, lc].astype(F32))
        ).astype(BF)
        if k < LEAD:
            spread_own(s, i)

    for w in wcopies[2:-1]:
        w.wait()
    ft = tile_of(FW)
    square = jnp.zeros((R, 1), F32)
    for k in range(len(order) + 1):
        if k < len(order):
            relay(*order[k])
            if k + LEAD < len(order):
                spread_own(*order[k + LEAD])
        if k == 0:
            continue
        s, i = order[k - 1]
        for kind in (1, 2, 4, 5):
            ag_copies[s, i, kind].wait_recv()
        at = (s * half + i * SW, s * half + DW + i * SW)
        xs = []
        for a in at:
            x = gath[:, a:a + SW].astype(F32)
            square = square + jnp.sum(x * x, axis=1, keepdims=True)
            xs.append((x * gain[:, a:a + SW]).astype(BF))

        def step(t, carry, xs=xs, at=at, k=k):
            fs = pl.ds(pl.multiple_of(t * ft, ft), ft)
            for acc, w in ((accg, wg), (accu, wu)):
                y = jnp.dot(xs[0], w[at[0]:at[0] + SW, fs], preferred_element_type=F32)
                y = y + jnp.dot(xs[1], w[at[1]:at[1] + SW, fs], preferred_element_type=F32)
                acc[:, fs] = y + acc[:, fs] if k > 1 else y
            return carry

        lax.fori_loop(0, FW // ft, step, 0)
    r = lax.rsqrt(square / D + 1e-5)

    def act(t, carry):
        fs = pl.ds(pl.multiple_of(t * ft, ft), ft)
        g = accg[:, fs] * r
        u = accu[:, fs] * r
        inner[:, fs] = (g / (1.0 + jnp.exp(-g)) * u).astype(BF)
        return carry

    lax.fori_loop(0, FW // ft, act, 0)
    wcopies[-1].wait()

    HW = CW // 2

    def halves(i):
        return pl.ds(i * CW, HW), pl.ds(i * CW + HW, HW)

    copies = {}

    def send(i, sem, rows, place, cs, to):
        cp = remote(part.at[rows, cs], rs.at[place, :, cs], r2_s.at[sem, i], r2_r.at[sem, i], "head", to)
        cp.start()
        copies[sem, i] = cp

    ct = tile_of(CW)
    for i in range(RCHUNKS):
        for t in range(CW // ct):
            cs = slice(i * CW + t * ct, i * CW + (t + 1) * ct)
            part[:, cs] = jnp.dot(inner[...], wd[:, cs], preferred_element_type=F32).astype(BF)
        ha, hb = halves(i)
        send(i, 0, rows_of(dg), 1, ha, nx)
        send(i, 1, rows_of(dg), 1, hb, ny)
        send(i, 2, rows_of(nx), 0, ha, nx)
        send(i, 3, rows_of(ny), 0, hb, ny)
    for i in range(RCHUNKS + 1):
        if i < RCHUNKS:
            ha, hb = halves(i)
            for cs, sem, to in ((ha, 0, ny), (hb, 1, nx)):
                copies[sem, i].wait_recv()
                rows = rows_of(to)
                part[rows, cs] = (part[rows, cs].astype(F32) + rs[1, :, cs].astype(F32)).astype(BF)
                send(i, 4 + sem, rows, 2, cs, to)
        if i:
            cs = pl.ds((i - 1) * CW, CW)
            for sem in (2, 3, 4, 5):
                copies[sem, i - 1].wait_recv()
            total = part[my_rows, cs].astype(F32)
            for place in (0, 2):
                total = total + rs[place, :, cs].astype(F32)
            out[:, cs] = (gath[my_rows, cs].astype(F32) + total).astype(BF)

    for cps in a_copies:
        for cp in cps:
            cp.wait_send()
    for cp in (*x_copies, *share, *at_copies, *o_copies.values(), *ag_copies.values(), *copies.values()):
        cp.wait_send()
    for g, t in own:
        @pl.when(j < J - 1)
        def _():
            z_copy(b, g, t).wait_send()

        @pl.when(c == 0)
        def _():
            d_copy(b, g, t).wait_send()

    def drain(s, carry):
        slot = 2 * (j - 1 - s) + c
        for g, t in own:
            @pl.when(j < J - 1)
            def _():
                z_copy(slot, g, t).wait_send()

            d_copy(slot, g, t).wait_send()
        return carry

    lax.fori_loop(0, j, drain, 0)


def square_call(H, B, hid, q, k, v, wo, gain, wg, wu, wd):
    T, D = hid.shape
    R = T * H
    QW = q.shape[1] // H
    G = k.shape[1] // H // HEAD_DIM
    FW = wg.shape[1]
    ratio = QW // HEAD_DIM // G
    AW = max(FW, D // 4, 2 * QW)
    vm = pl.BlockSpec(memory_space=pltpu.VMEM)
    hbm = pl.BlockSpec(memory_space=pl.ANY)
    dma = pltpu.SemaphoreType.DMA
    return pl.pallas_call(
        functools.partial(square_kernel, H, B),
        out_shape=jax.ShapeDtypeStruct((T, D), BF),
        in_specs=[vm] * 5 + [hbm] * 4,
        out_specs=vm,
        scratch_shapes=[
            pltpu.VMEM((2, 2 * QW, D // 4), BF),
            pltpu.VMEM(wg.shape, BF),
            pltpu.VMEM(wu.shape, BF),
            pltpu.VMEM(wd.shape, BF),
            pltpu.VMEM((G, ratio * R, HEAD_DIM), BF),
            pltpu.VMEM((B, G, 2, R, HEAD_DIM), BF),
            pltpu.VMEM((R, QW), BF),
            pltpu.VMEM((2, R, QW), BF),
            pltpu.VMEM((2, T, D // 4), BF),
            pltpu.VMEM((2, 2 * T, D // 4), BF),
            pltpu.VMEM((2, 2 * T, D // 4), BF),
            pltpu.VMEM((R, D), BF),
            pltpu.VMEM((3, T, D), BF),
            pltpu.VMEM((R, D), BF),
            pltpu.VMEM((R, AW), F32),
            pltpu.VMEM((R, AW), F32),
            pltpu.VMEM((R, FW), BF),
            dma((3 + 2 * CHUNKS,)),
            dma((H - 1, G * (2 + ratio))), dma((H - 1, G * (2 + ratio))),
            dma((B, G, 2)), dma((B, G, 2)),
            dma((B, G, 2)), dma((B, G, 2)),
            dma((6,)), dma((6,)),
            dma((G, 2)), dma((G, 2)),
            dma((2, SUBS)), dma((2, SUBS)),
            dma((2, SUBS, 6)), dma((2, SUBS, 6)),
            dma((6, RCHUNKS)), dma((6, RCHUNKS)),
        ],
        compiler_params=pltpu.CompilerParams(
            collective_id=0, has_side_effects=True, vmem_limit_bytes=67_043_328
        ),
    )(hid, q, k, v, gain.reshape(1, -1), wo, wg, wu, wd)


def solution(mesh):
    H = mesh.shape["head"]
    B = mesh.shape["blk"]

    def local(hid, q, k, v, wo, gain, wg, wu, wd):
        if H == 4:
            return square_call(H, B, hid, q, k, v, wo, gain, wg, wu, wd)
        T, D = hid.shape
        R = T * H
        QW = q.shape[1] // H
        KW = k.shape[1] // H
        FW = wg.shape[1]
        vm = pl.BlockSpec(memory_space=pltpu.VMEM)
        hbm = pl.BlockSpec(memory_space=pl.ANY)
        dma = pltpu.SemaphoreType.DMA
        return pl.pallas_call(
            functools.partial(general_kernel, H, B),
            out_shape=jax.ShapeDtypeStruct((T, D), BF),
            in_specs=[vm] * 5 + [hbm] * 4,
            out_specs=vm,
            scratch_shapes=[
                pltpu.VMEM(wo.shape, BF),
                pltpu.VMEM(wg.shape, BF),
                pltpu.VMEM(wu.shape, BF),
                pltpu.VMEM(wd.shape, BF),
                pltpu.VMEM((R, QW), BF),
                pltpu.VMEM((B, 2, R, KW), BF),
                pltpu.VMEM((R, QW), BF),
                pltpu.VMEM((R, D), BF),
                pltpu.VMEM((H - 1, T, D), BF),
                pltpu.VMEM((R, D), BF),
                pltpu.VMEM((R, FW), F32),
                pltpu.VMEM((R, FW), F32),
                pltpu.VMEM((R, FW), BF),
                dma((2 + 2 * CHUNKS,)),
                dma((3,)),
                dma((H - 1, 3)), dma((H - 1, 3)),
                dma((B, 2)), dma((B, 2)),
                dma((B, 2)), dma((B, 2)),
                dma((max(H - 1, 6), CHUNKS)), dma((max(H - 1, 6), CHUNKS)),
                dma((max(H - 1, 6), CHUNKS)), dma((max(H - 1, 6), CHUNKS)),
                dma((max(H - 1, 6), CHUNKS)), dma((max(H - 1, 6), CHUNKS)),
            ],
            compiler_params=pltpu.CompilerParams(
                collective_id=0, has_side_effects=True, vmem_limit_bytes=67_043_328
            ),
        )(hid, q, k, v, gain.reshape(1, -1), wo, wg, wu, wd)

    rows = P(("blk", "head"), None)
    return jax.shard_map(
        local,
        mesh=mesh,
        in_specs=(rows, rows, rows, rows, P("head", None), P(), P(None, "head"), P(None, "head"), P("head", None)),
        out_specs=rows,
        check_vma=False,
    )
```

```python
import functools

import jax
import jax.numpy as jnp
from jax import lax
from jax.experimental import pallas as pl
from jax.experimental.pallas import tpu as pltpu
from jax.sharding import PartitionSpec as P

HEADS = 16
KV_HEADS = 8
HEAD_DIM = 128
CHUNKS = 4
AHEAD = 2
SUBS = 4
LEAD = 3
LAG = 3
QB = 128
WIDTHS = (1, 1, 2, 2, 2)
LOG2E = 1.4426950408889634
MESH = pl.DeviceIdType.MESH
BF = jnp.bfloat16
F32 = jnp.float32


def tile_of(n, most=256):
    t = most
    while n % t:
        t -= 128
    return t


def remote(src, dst, send, recv, axis, index):
    return pltpu.make_async_remote_copy(
        src_ref=src, dst_ref=dst, send_sem=send, recv_sem=recv,
        device_id={axis: index}, device_id_type=MESH,
    )


def general_kernel(
    H, B,
    hid, q_in, k_in, v_in, gain, wo_h, wg_h, wu_h, wd_h,
    out,
    wo, wg, wu, wd, qb, kv, att, part, rs, gath, accg, accu, inner,
    w_sem, loc_sem, a_s, a_r, z_s, z_r, d_s, d_r, rs_s, rs_r, ag_s, ag_r, r2_s, r2_r,
):
    h = lax.axis_index("head")
    b = lax.axis_index("blk")
    J = B // 2
    j = b // 2
    c = b % 2
    partner = b + 1 - 2 * c
    T = hid.shape[0]
    D = hid.shape[1]
    R = T * H
    QW = qb.shape[1]
    KW = kv.shape[3]
    nh = QW // HEAD_DIM
    ratio = HEADS // KV_HEADS
    CW = D // CHUNKS
    FW = wg.shape[1]

    wcopies = [pltpu.make_async_copy(wo_h, wo, w_sem.at[0])]
    for i in range(CHUNKS):
        rows = pl.ds(i * CW, CW)
        wcopies.append(pltpu.make_async_copy(wg_h.at[rows], wg.at[rows], w_sem.at[1 + 2 * i]))
        wcopies.append(pltpu.make_async_copy(wu_h.at[rows], wu.at[rows], w_sem.at[2 + 2 * i]))
    wcopies.append(pltpu.make_async_copy(wd_h, wd, w_sem.at[1 + 2 * CHUNKS]))
    barrier = pltpu.get_barrier_semaphore()
    for d in range(1, H):
        pl.semaphore_signal(barrier, inc=1, device_id={"head": lax.rem(h + d, H)}, device_id_type=MESH)

    @pl.when(j > 0)
    def _():
        pl.semaphore_signal(barrier, inc=1, device_id={"blk": lax.rem(b + B - 2, B)}, device_id_type=MESH)

    @pl.when(j < J - 1)
    def _():
        pl.semaphore_signal(barrier, inc=1, device_id={"blk": lax.rem(b + 2, B)}, device_id_type=MESH)

    pl.semaphore_signal(barrier, inc=1, device_id={"blk": partner}, device_id_type=MESH)
    pl.semaphore_wait(barrier, H + jnp.minimum(j, 1) + jnp.minimum(J - 1 - j, 1))

    my_rows = pl.ds(pl.multiple_of(h * T, T), T)

    def cols(p, w):
        return pl.ds(pl.multiple_of(p * w, w), w)

    a_copies = []
    for t, (src, dst, w) in enumerate(
        ((k_in, kv.at[b, 0], KW), (v_in, kv.at[b, 1], KW), (q_in, qb, QW))
    ):
        for d in range(1, H):
            p = lax.rem(h + d, H)
            cp = remote(
                src.at[:, cols(p, w)], dst.at[my_rows, :],
                a_s.at[d - 1, t], a_r.at[d - 1, t], "head", p,
            )
            cp.start()
            a_copies.append((t, cp))
        lc = pltpu.make_async_copy(src.at[:, cols(h, w)], dst.at[my_rows, :], loc_sem.at[t])
        lc.start()
        a_copies.append((t, lc))

    def wait_in(t):
        for tt, cp in a_copies:
            if tt == t:
                cp.wait()

    def z_copy(slot, t):
        return remote(
            kv.at[slot, t], kv.at[slot, t], z_s.at[slot, t], z_r.at[slot, t],
            "blk", lax.rem(b + 2, B),
        )

    def d_copy(slot, t):
        return remote(
            kv.at[slot, t], kv.at[slot, t], d_s.at[slot, t], d_r.at[slot, t], "blk", partner
        )

    for t in range(2):
        wait_in(t)

        @pl.when(j < J - 1)
        def _():
            z_copy(b, t).start()

        @pl.when(c == 0)
        def _():
            d_copy(b, t).start()

    wait_in(2)
    for w in wcopies:
        w.start()

    mq = lambda n: slice(n * HEAD_DIM, (n + 1) * HEAD_DIM)
    ml = lambda n: slice((nh + n) * HEAD_DIM, (nh + n + 1) * HEAD_DIM)
    scale = HEAD_DIM ** (-0.5)

    def absorb(slot, first):
        for n in range(nh):
            g = n // ratio
            s = lax.dot_general(
                qb[:, mq(n)], kv[slot, 0, :, mq(g)],
                (((1,), (1,)), ((), ())), preferred_element_type=F32,
            ) * scale
            if first:
                qi = lax.broadcasted_iota(jnp.int32, s.shape, 0)
                ki = lax.broadcasted_iota(jnp.int32, s.shape, 1)
                s = jnp.where(ki <= qi, s, -1e30)
            top = jnp.max(s, axis=1, keepdims=True)
            if not first:
                old = accu[:, mq(n)][:, :1]
                top = jnp.maximum(top, old)
            e = jnp.exp(s - top)
            tot = jnp.sum(e, axis=1, keepdims=True)
            pv = jnp.dot(e.astype(BF), kv[slot, 1, :, mq(g)], preferred_element_type=F32)
            if not first:
                f = jnp.exp(old - top)
                tot = tot + accu[:, ml(n)][:, :1] * f
                pv = pv + accg[:, mq(n)] * f
            accu[:, mq(n)] = jnp.broadcast_to(top, (R, HEAD_DIM))
            accu[:, ml(n)] = jnp.broadcast_to(tot, (R, HEAD_DIM))
            accg[:, mq(n)] = pv

    absorb(b, True)

    @pl.when(c == 1)
    def _():
        for t in range(2):
            d_copy(b - 1, t).wait_recv()
        absorb(b - 1, False)

    def chain(s, carry):
        slot = 2 * (j - 1 - s) + c
        other = 2 * (j - 1 - s) + 1 - c
        for t in range(2):
            z_copy(slot, t).wait_recv()

            @pl.when(j < J - 1)
            def _():
                z_copy(slot, t).start()

            d_copy(slot, t).start()
        absorb(slot, False)
        for t in range(2):
            d_copy(other, t).wait_recv()
        absorb(other, False)
        return carry

    lax.fori_loop(0, j, chain, 0)

    for n in range(nh):
        att[:, mq(n)] = (accg[:, mq(n)] / accu[:, ml(n)]).astype(BF)

    square_ring = H == 4
    nx = h + 1 - 2 * (h % 2)
    ny = lax.rem(h + H // 2, H)
    dg = H - 1 - h
    HW = CW // 2

    def rows_of(p):
        return pl.ds(pl.multiple_of(p * T, T), T)

    def halves(i):
        return pl.ds(i * CW, HW), pl.ds(i * CW + HW, HW)

    def scatter(w_ref, x_ref, send, recv):
        copies = {}
        ct = tile_of(CW)
        for i in range(CHUNKS):
            def step(t, carry):
                cs = pl.ds(pl.multiple_of(i * CW + t * ct, ct), ct)
                part[:, cs] = jnp.dot(
                    x_ref[...], w_ref[:, cs], preferred_element_type=F32
                ).astype(BF)
                return carry

            lax.fori_loop(0, CW // ct, step, 0)
            if square_ring:
                ha, hb = halves(i)
                plan = ((1, dg, ha, 0, nx), (1, dg, hb, 1, ny), (0, nx, ha, 2, nx), (0, ny, hb, 3, ny))
            else:
                cs = pl.ds(i * CW, CW)
                plan = [(d - 1, lax.rem(h + d, H), cs, d - 1, lax.rem(h + d, H)) for d in range(1, H)]
            for place, block, cs, sem, to in plan:
                cp = remote(
                    part.at[rows_of(block), cs], rs.at[place, :, cs],
                    send.at[sem, i], recv.at[sem, i], "head", to,
                )
                cp.start()
                copies[sem, i] = cp
        return copies

    def combine(i, copies, send, recv):
        if not square_ring:
            return
        ha, hb = halves(i)
        for cs, sem, to in ((ha, 0, ny), (hb, 1, nx)):
            copies[sem, i].wait_recv()
            blk_rows = rows_of(to)
            part[blk_rows, cs] = (
                part[blk_rows, cs].astype(F32) + rs[1, :, cs].astype(F32)
            ).astype(BF)
            cp = remote(
                part.at[blk_rows, cs], rs.at[2, :, cs],
                send.at[4 + sem, i], recv.at[4 + sem, i], "head", to,
            )
            cp.start()
            copies[4 + sem, i] = cp

    def reduced(i, copies):
        cs = pl.ds(i * CW, CW)
        sems = (2, 3, 4, 5) if square_ring else range(H - 1)
        for sem in sems:
            copies[sem, i].wait_recv()
        total = part[my_rows, cs].astype(F32)
        for place in (0, 2) if square_ring else range(H - 1):
            total = total + rs[place, :, cs].astype(F32)
        return total

    wcopies[0].wait()
    rs_copies = scatter(wo, att, rs_s, rs_r)
    ag_copies = {}

    def spread(rows, cs, sem, i, to):
        cp = remote(
            gath.at[rows, cs], gath.at[rows, cs],
            ag_s.at[sem, i], ag_r.at[sem, i], "head", to,
        )
        cp.start()
        ag_copies[sem, i] = cp

    def spread_own(i):
        for sem, to in enumerate(
            (nx, ny) if square_ring else [lax.rem(h + d, H) for d in range(1, H)]
        ):
            spread(my_rows, pl.ds(i * CW, CW), sem, i, to)

    for i in range(CHUNKS + 1):
        if i < CHUNKS:
            combine(i, rs_copies, rs_s, rs_r)
        if i:
            cs = pl.ds((i - 1) * CW, CW)
            gath[my_rows, cs] = (hid[:, cs].astype(F32) + reduced(i - 1, rs_copies)).astype(BF)
            if i <= AHEAD or not square_ring:
                spread_own(i - 1)

    ft = tile_of(FW)
    square = jnp.zeros((R, 1), F32)
    for i in range(CHUNKS + 1):
        if i < CHUNKS and square_ring:
            ha, hb = halves(i)
            ag_copies[0, i].wait_recv()
            spread(rows_of(nx), ha, 2, i, ny)
            ag_copies[1, i].wait_recv()
            spread(rows_of(ny), hb, 3, i, nx)
            if i + AHEAD < CHUNKS:
                spread_own(i + AHEAD)
        if i == 0:
            continue
        k = i - 1
        cs = pl.ds(k * CW, CW)
        for sem in (2, 3) if square_ring else range(H - 1):
            ag_copies[sem, k].wait_recv()
        wcopies[1 + 2 * k].wait()
        wcopies[2 + 2 * k].wait()
        x = gath[:, cs].astype(F32)
        square = square + jnp.sum(x * x, axis=1, keepdims=True)
        xg = (x * gain[:, cs]).astype(BF)

        def step(t, carry, xg=xg, cs=cs, k=k):
            fs = pl.ds(pl.multiple_of(t * ft, ft), ft)
            g = jnp.dot(xg, wg[cs, fs], preferred_element_type=F32)
            u = jnp.dot(xg, wu[cs, fs], preferred_element_type=F32)
            if k:
                g = g + accg[:, fs]
                u = u + accu[:, fs]
            accg[:, fs] = g
            accu[:, fs] = u
            return carry

        lax.fori_loop(0, FW // ft, step, 0)
    r = lax.rsqrt(square / D + 1e-5)

    def act(t, carry):
        fs = pl.ds(pl.multiple_of(t * ft, ft), ft)
        g = accg[:, fs] * r
        u = accu[:, fs] * r
        inner[:, fs] = (g / (1.0 + jnp.exp(-g)) * u).astype(BF)
        return carry

    lax.fori_loop(0, FW // ft, act, 0)
    for cp in rs_copies.values():
        cp.wait_send()
    wcopies[-1].wait()
    r2_copies = scatter(wd, inner, r2_s, r2_r)
    for i in range(CHUNKS + 1):
        if i < CHUNKS:
            combine(i, r2_copies, r2_s, r2_r)
        if i:
            cs = pl.ds((i - 1) * CW, CW)
            out[:, cs] = (gath[my_rows, cs].astype(F32) + reduced(i - 1, r2_copies)).astype(BF)

    for cp in (*ag_copies.values(), *r2_copies.values()):
        cp.wait_send()
    for t in range(2):
        @pl.when(j < J - 1)
        def _():
            z_copy(b, t).wait_send()

        @pl.when(c == 0)
        def _():
            d_copy(b, t).wait_send()

    def drain(s, carry):
        slot = 2 * (j - 1 - s) + c
        for t in range(2):
            @pl.when(j < J - 1)
            def _():
                z_copy(slot, t).wait_send()

            d_copy(slot, t).wait_send()
        return carry

    lax.fori_loop(0, j, drain, 0)


def square_kernel(
    H, B,
    hid, q_in, k_in, v_in, gain, wo_h, wg_h, wu_h, wd_h,
    out,
    wo, wg, wu, wd, qb, kv, att, attx, hx, sb, rb, part, rs, gath, accg, accu, inner,
    w_sem, a_s, a_r, z_s, z_r, d_s, d_r, x_s, x_r, at_s, at_r, o_s, o_r, ag_s, ag_r, r2_s, r2_r,
):
    h = lax.axis_index("head")
    b = lax.axis_index("blk")
    J = B // 2
    j = b // 2
    c = b % 2
    partner = b + 1 - 2 * c
    T, D = hid.shape
    R = T * H
    G = kv.shape[1]
    QW = qb.shape[1]
    ratio = QW // G // HEAD_DIM
    GW = QW // G
    FW = wg.shape[1]
    half = D // 2
    DW = D // 4
    SW = DW // SUBS

    ex, ey = h % 2, h // 2
    nx = h + 1 - 2 * ex
    ny = lax.rem(h + 2, H)
    dg = H - 1 - h
    pair = (nx, ny)
    across = (ny, nx)
    mine = (ex, ey)

    wcopies = []
    for s in range(2):
        src = wo_h.at[:, pl.ds(pl.multiple_of(s * half + mine[s] * DW, DW), DW)]
        wcopies.append((src, wo.at[s, pl.ds(0, QW)]))
    for i in range(CHUNKS):
        rows = pl.ds(i * (D // CHUNKS), D // CHUNKS)
        wcopies.append((wg_h.at[rows], wg.at[rows]))
        wcopies.append((wu_h.at[rows], wu.at[rows]))
    wcopies.append((wd_h, wd))
    wcopies = [pltpu.make_async_copy(s, d, w_sem.at[n]) for n, (s, d) in enumerate(wcopies)]

    barrier = pltpu.get_barrier_semaphore()
    for d in range(1, H):
        pl.semaphore_signal(barrier, inc=1, device_id={"head": lax.rem(h + d, H)}, device_id_type=MESH)

    @pl.when(j > 0)
    def _():
        pl.semaphore_signal(barrier, inc=1, device_id={"blk": lax.rem(b + B - 2, B)}, device_id_type=MESH)

    @pl.when(j < J - 1)
    def _():
        pl.semaphore_signal(barrier, inc=1, device_id={"blk": lax.rem(b + 2, B)}, device_id_type=MESH)

    pl.semaphore_signal(barrier, inc=1, device_id={"blk": partner}, device_id_type=MESH)
    pl.semaphore_wait(barrier, H + jnp.minimum(j, 1) + jnp.minimum(J - 1 - j, 1))

    def rows_of(p):
        return pl.ds(pl.multiple_of(p * T, T), T)

    my_rows = rows_of(h)

    pieces = []
    for g in range(G):
        pieces.append((k_in, G, g, kv.at[b, g, 0, my_rows, :]))
        pieces.append((v_in, G, g, kv.at[b, g, 1, my_rows, :]))
    pieces.append((q_in, 1, 0, qb.at[my_rows, :]))

    def piece_cols(p, per, n, dst):
        w = dst.shape[1]
        return pl.ds(pl.multiple_of((p * per + n) * w, w), w)

    a_copies = []
    for t, (src, per, n, dst) in enumerate(pieces):
        cps = []
        for d, p in enumerate((dg, nx, ny)):
            cp = remote(src.at[:, piece_cols(p, per, n, dst)], dst, a_s.at[d, t], a_r.at[d, t], "head", p)
            cp.start()
            cps.append(cp)
        a_copies.append(cps)

    x_copies = []
    for s in range(2):
        cs = pl.ds(pl.multiple_of(s * half + (1 - mine[s]) * DW, DW), DW)
        x_copies.append(remote(hid.at[:, cs], hx.at[s], x_s.at[s], x_r.at[s], "head", pair[s]))
    core_cols = pl.ds(pl.multiple_of(c * (DW // 2), DW // 2), DW // 2)
    for s in range(2):
        cs = pl.ds(pl.multiple_of(s * half + (1 - mine[s]) * DW + c * (DW // 2), DW // 2), DW // 2)
        x_copies.append(remote(
            wo_h.at[:, cs], wo.at[s, pl.ds(QW, QW), core_cols],
            x_s.at[2 + s], x_r.at[2 + s], "head", pair[s],
        ))
    for cp in x_copies:
        cp.start()
    share = []
    for s in range(2):
        ref = wo.at[s, pl.ds(QW, QW), core_cols]
        share.append(remote(ref, ref, x_s.at[4 + s], x_r.at[4 + s], "blk", partner))

    for t, (src, per, n, dst) in enumerate(pieces):
        dst[...] = src[:, piece_cols(h, per, n, dst)]

    def wait_in(t):
        for cp in a_copies[t]:
            cp.wait_recv()

    def z_copy(slot, g, t):
        ref = kv.at[slot, g, t]
        return remote(ref, ref, z_s.at[slot, g, t], z_r.at[slot, g, t], "blk", lax.rem(b + 2, B))

    def d_copy(slot, g, t):
        ref = kv.at[slot, g, t]
        return remote(ref, ref, d_s.at[slot, g, t], d_r.at[slot, g, t], "blk", partner)

    own = [(g, t) for g in range(G) for t in range(2)]
    for n, (g, t) in enumerate(own):
        wait_in(n)

        @pl.when((j < J - 1) & ((j == 0) | (n < len(own) - 1)))
        def _():
            z_copy(b, g, t).start()

        @pl.when(c == 0)
        def _():
            d_copy(b, g, t).start()

    def pass_on(slot, g, t):
        z_copy(slot, g, t).wait_recv()

        @pl.when(j < J - 1)
        def _():
            z_copy(slot, g, t).start()

        d_copy(slot, g, t).start()

    def both(s):
        first = 2 * (j - 1 - s)
        return first + c, first + 1 - c

    def pass_on_first(g):
        @pl.when(j > 0)
        def _():
            for t in range(2):
                pass_on(both(0)[0], g, t)

    pass_on_first(0)

    @pl.when((j > 0) & (j < J - 1))
    def _():
        z_copy(b, *own[-1]).start()

    wait_in(len(own))
    for w in wcopies:
        w.start()

    factor = HEAD_DIM ** (-0.5) * LOG2E

    def absorb(g, slots, first):
        ones = jnp.ones((R, HEAD_DIM), BF)
        keys = jnp.concatenate([kv[slot, g, 0] for slot in slots], axis=0)
        values = jnp.concatenate(
            [jnp.concatenate([kv[slot, g, 1], ones], axis=1) for slot in slots], axis=0
        )
        for r in range(ratio):
            n = g * ratio + r
            tops = slice(n * HEAD_DIM, (n + 1) * HEAD_DIM)
            sums = slice(2 * n * HEAD_DIM, 2 * (n + 1) * HEAD_DIM)
            for q0 in range(0, R, QB):
                rows = slice(q0, q0 + QB)
                sc = lax.dot_general(
                    qb[rows, tops], keys,
                    (((1,), (1,)), ((), ())), preferred_element_type=F32,
                )
                tiles = [sc[:, t:t + HEAD_DIM] for t in range(0, len(slots) * R, HEAD_DIM)]
                if first:
                    qi = q0 + lax.broadcasted_iota(jnp.int32, tiles[0].shape, 0)
                    ki = lax.broadcasted_iota(jnp.int32, tiles[0].shape, 1)
                    for t in range(R // HEAD_DIM):
                        tiles[t] = jnp.where(ki + t * HEAD_DIM <= qi, tiles[t], -1e30)
                top = functools.reduce(jnp.maximum, tiles)
                top = jnp.broadcast_to(jnp.max(top, axis=1, keepdims=True), top.shape)
                if not first:
                    old = accu[rows, tops]
                    top = jnp.maximum(top, old)
                peak = top * factor
                e = jnp.concatenate([jnp.exp2(t * factor - peak).astype(BF) for t in tiles], axis=1)
                pv = jnp.dot(e, values, preferred_element_type=F32)
                if not first:
                    f = jnp.exp2(old * factor - peak)
                    pv = pv + accg[rows, sums] * jnp.concatenate([f, f], axis=1)
                accu[rows, tops] = top
                accg[rows, sums] = pv

    for g in range(G):
        @pl.when(c == 0)
        def _(g=g):
            absorb(g, (b,), True)

        @pl.when(c == 1)
        def _(g=g):
            for t in range(2):
                d_copy(b - 1, g, t).wait_recv()
            absorb(g, (b, b - 1), True)

    at_copies = []
    for g in range(G):
        def chain(s, carry, g=g):
            slot, other = both(s)

            @pl.when(s > 0)
            def _():
                for t in range(2):
                    pass_on(slot, g, t)

            for t in range(2):
                d_copy(other, g, t).wait_recv()
            absorb(g, (slot, other), False)
            return carry

        lax.fori_loop(0, j, chain, 0)
        if g + 1 < G:
            pass_on_first(g + 1)
        for r in range(ratio):
            n = g * ratio + r
            pv = accg[:, 2 * n * HEAD_DIM:2 * (n + 1) * HEAD_DIM]
            att[:, n * HEAD_DIM:(n + 1) * HEAD_DIM] = (pv[:, :HEAD_DIM] / pv[:, HEAD_DIM:]).astype(BF)
        cs = pl.ds(g * GW, GW)
        for s in range(2):
            cp = remote(att.at[:, cs], attx.at[s, :, cs], at_s.at[g, s], at_r.at[g, s], "head", pair[s])
            cp.start()
            at_copies.append(cp)

    accs = (accg, accu)
    for s in range(2):
        x_copies[2 + s].wait_recv()
        share[s].start()
    for s in range(2):
        wcopies[s].wait()
        for t in range(SUBS):
            cs = slice(t * SW, (t + 1) * SW)
            accs[s][:, cs] = jnp.dot(att[...], wo[s, :QW, cs], preferred_element_type=F32)
    for s in range(2):
        share[s].wait_recv()
    for cp in at_copies:
        cp.wait_recv()

    co = ({"h": nx, "x": h, "y": dg, "d": ny}, {"h": ny, "x": dg, "y": h, "d": nx})
    order = [(s, i) for i in range(SUBS) for s in range(2)]
    o_copies = {}
    for s, i in order:
        cs = pl.ds(i * SW, SW)
        accs[s][:, cs] += jnp.dot(attx[s], wo[s, QW:, i * SW:(i + 1) * SW], preferred_element_type=F32)
        to = across[s]
        away = (to, co[s]["y" if s == 0 else "x"])
        for n, p in enumerate(away):
            sb[s, n * T:(n + 1) * T, i * SW:(i + 1) * SW] = accs[s][rows_of(p), cs].astype(BF)
        cp = remote(sb.at[s, :, cs], rb.at[s, :, cs], o_s.at[s, i], o_r.at[s, i], "head", to)
        cp.start()
        o_copies[s, i] = cp

    def cols_of(s, i, other):
        part_index = 1 - mine[s] if other else mine[s]
        return pl.ds(pl.multiple_of(s * half + part_index * DW + i * SW, SW), SW)

    ag_copies = {}

    def spread(s, i, kind, rows, cs, to):
        ref = gath.at[rows, cs]
        cp = remote(ref, ref, ag_s.at[s, i, kind], ag_r.at[s, i, kind], "head", to)
        cp.start()
        ag_copies[s, i, kind] = cp

    def spread_own(s, i):
        cs = cols_of(s, i, False)
        for n, to in enumerate((nx, ny)):
            spread(s, i, 2 * n, my_rows, cs, to)
            spread(s, i, 2 * n + 1, rows_of(co[s]["h"]), cs, to)

    def relay(s, i):
        ag_copies[s, i, 0].wait_recv()
        spread(s, i, 4, rows_of(nx), cols_of(s, i, s == 0), ny)
        ag_copies[s, i, 3].wait_recv()
        spread(s, i, 5, rows_of(co[s]["y"]), cols_of(s, i, s == 1), nx)

    for s in range(2):
        x_copies[s].wait_recv()
    for k, (s, i) in enumerate(order):
        o_copies[s, i].wait_recv()
        cs = cols_of(s, i, False)
        lc = slice(i * SW, (i + 1) * SW)
        gath[my_rows, cs] = (
            hid[:, cs].astype(F32) + (accs[s][my_rows, lc] + rb[s, :T, lc].astype(F32))
        ).astype(BF)
        cr = rows_of(co[s]["h"])
        gath[cr, cs] = (
            hx[s, :, lc].astype(F32) + (accs[s][cr, lc] + rb[s, T:, lc].astype(F32))
        ).astype(BF)
        if k < LEAD:
            spread_own(s, i)

    for w in wcopies[2:-1]:
        w.wait()
    ft = tile_of(FW)
    square = jnp.zeros((R, 1), F32)
    for n in range(len(order) + LAG):
        if n < len(order):
            relay(*order[n])
            if n + LEAD < len(order):
                spread_own(*order[n + LEAD])
        if n < LAG:
            continue
        k = n - LAG
        s, i = order[k]
        for kind in (1, 2, 4, 5):
            ag_copies[s, i, kind].wait_recv()
        at = (s * half + i * SW, s * half + DW + i * SW)
        xs = []
        for a in at:
            x = gath[:, a:a + SW].astype(F32)
            square = square + jnp.sum(x * x, axis=1, keepdims=True)
            xs.append((x * gain[:, a:a + SW]).astype(BF))

        last = k == len(order) - 1
        if last:
            r = lax.rsqrt(square / D + 1e-5)
        for t in range(FW // ft):
            fs = slice(t * ft, (t + 1) * ft)
            ys = []
            for acc, w in ((accg, wg), (accu, wu)):
                y = jnp.dot(xs[0], w[at[0]:at[0] + SW, fs], preferred_element_type=F32)
                y = y + jnp.dot(xs[1], w[at[1]:at[1] + SW, fs], preferred_element_type=F32)
                if k:
                    y = y + acc[:, fs]
                if last:
                    ys.append(y * r)
                else:
                    acc[:, fs] = y
            if last:
                g, u = ys
                inner[:, fs] = (g / (1.0 + jnp.exp(-g)) * u).astype(BF)
    wcopies[-1].wait()

    unit = D // sum(WIDTHS)
    spans = [(sum(WIDTHS[:i]) * unit, w * unit) for i, w in enumerate(WIDTHS)]

    def halves(i):
        at, w = spans[i]
        return pl.ds(at, w // 2), pl.ds(at + w // 2, w // 2)

    copies = {}

    def send(i, sem, rows, place, cs, to):
        cp = remote(part.at[rows, cs], rs.at[place, :, cs], r2_s.at[sem, i], r2_r.at[sem, i], "head", to)
        cp.start()
        copies[sem, i] = cp

    for i, (at, w) in enumerate(spans):
        ct = tile_of(w)
        for t in range(w // ct):
            cs = slice(at + t * ct, at + (t + 1) * ct)
            part[:, cs] = jnp.dot(inner[...], wd[:, cs], preferred_element_type=F32).astype(BF)
        ha, hb = halves(i)
        send(i, 0, rows_of(dg), 1, ha, nx)
        send(i, 1, rows_of(dg), 1, hb, ny)
        send(i, 2, rows_of(nx), 0, ha, nx)
        send(i, 3, rows_of(ny), 0, hb, ny)
    for i in range(len(spans)):
        ha, hb = halves(i)
        for cs, sem, to in ((ha, 0, ny), (hb, 1, nx)):
            copies[sem, i].wait_recv()
            rows = rows_of(to)
            part[rows, cs] = (part[rows, cs].astype(F32) + rs[1, :, cs].astype(F32)).astype(BF)
            send(i, 4 + sem, rows, 2, cs, to)
    for i in range(len(spans)):
        cs = pl.ds(*spans[i])
        for sem in (2, 3, 4, 5):
            copies[sem, i].wait_recv()
        total = part[my_rows, cs].astype(F32)
        for place in (0, 2):
            total = total + rs[place, :, cs].astype(F32)
        out[:, cs] = (gath[my_rows, cs].astype(F32) + total).astype(BF)

    for cps in a_copies:
        for cp in cps:
            cp.wait_send()
    for cp in (*x_copies, *share, *at_copies, *o_copies.values(), *ag_copies.values(), *copies.values()):
        cp.wait_send()
    for g, t in own:
        @pl.when(j < J - 1)
        def _():
            z_copy(b, g, t).wait_send()

        @pl.when(c == 0)
        def _():
            d_copy(b, g, t).wait_send()

    def drain(s, carry):
        slot = 2 * (j - 1 - s) + c
        for g, t in own:
            @pl.when(j < J - 1)
            def _():
                z_copy(slot, g, t).wait_send()

            d_copy(slot, g, t).wait_send()
        return carry

    lax.fori_loop(0, j, drain, 0)


def square_call(H, B, hid, q, k, v, wo, gain, wg, wu, wd):
    T, D = hid.shape
    R = T * H
    QW = q.shape[1] // H
    G = k.shape[1] // H // HEAD_DIM
    FW = wg.shape[1]
    ratio = QW // HEAD_DIM // G
    AW = max(FW, D // 4, 2 * QW)
    vm = pl.BlockSpec(memory_space=pltpu.VMEM)
    hbm = pl.BlockSpec(memory_space=pl.ANY)
    dma = pltpu.SemaphoreType.DMA
    return pl.pallas_call(
        functools.partial(square_kernel, H, B),
        out_shape=jax.ShapeDtypeStruct((T, D), BF),
        in_specs=[vm] * 5 + [hbm] * 4,
        out_specs=vm,
        scratch_shapes=[
            pltpu.VMEM((2, 2 * QW, D // 4), BF),
            pltpu.VMEM(wg.shape, BF),
            pltpu.VMEM(wu.shape, BF),
            pltpu.VMEM(wd.shape, BF),
            pltpu.VMEM((R, QW), BF),
            pltpu.VMEM((B, G, 2, R, HEAD_DIM), BF),
            pltpu.VMEM((R, QW), BF),
            pltpu.VMEM((2, R, QW), BF),
            pltpu.VMEM((2, T, D // 4), BF),
            pltpu.VMEM((2, 2 * T, D // 4), BF),
            pltpu.VMEM((2, 2 * T, D // 4), BF),
            pltpu.VMEM((R, D), BF),
            pltpu.VMEM((3, T, D), BF),
            pltpu.VMEM((R, D), BF),
            pltpu.VMEM((R, AW), F32),
            pltpu.VMEM((R, AW), F32),
            pltpu.VMEM((R, FW), BF),
            dma((3 + 2 * CHUNKS,)),
            dma((H - 1, 2 * G + 1)), dma((H - 1, 2 * G + 1)),
            dma((B, G, 2)), dma((B, G, 2)),
            dma((B, G, 2)), dma((B, G, 2)),
            dma((6,)), dma((6,)),
            dma((G, 2)), dma((G, 2)),
            dma((2, SUBS)), dma((2, SUBS)),
            dma((2, SUBS, 6)), dma((2, SUBS, 6)),
            dma((6, len(WIDTHS))), dma((6, len(WIDTHS))),
        ],
        compiler_params=pltpu.CompilerParams(
            collective_id=0, has_side_effects=True, vmem_limit_bytes=67_043_328
        ),
    )(hid, q, k, v, gain.reshape(1, -1), wo, wg, wu, wd)


def solution(mesh):
    H = mesh.shape["head"]
    B = mesh.shape["blk"]

    def local(hid, q, k, v, wo, gain, wg, wu, wd):
        if H == 4:
            return square_call(H, B, hid, q, k, v, wo, gain, wg, wu, wd)
        T, D = hid.shape
        R = T * H
        QW = q.shape[1] // H
        KW = k.shape[1] // H
        FW = wg.shape[1]
        vm = pl.BlockSpec(memory_space=pltpu.VMEM)
        hbm = pl.BlockSpec(memory_space=pl.ANY)
        dma = pltpu.SemaphoreType.DMA
        return pl.pallas_call(
            functools.partial(general_kernel, H, B),
            out_shape=jax.ShapeDtypeStruct((T, D), BF),
            in_specs=[vm] * 5 + [hbm] * 4,
            out_specs=vm,
            scratch_shapes=[
                pltpu.VMEM(wo.shape, BF),
                pltpu.VMEM(wg.shape, BF),
                pltpu.VMEM(wu.shape, BF),
                pltpu.VMEM(wd.shape, BF),
                pltpu.VMEM((R, QW), BF),
                pltpu.VMEM((B, 2, R, KW), BF),
                pltpu.VMEM((R, QW), BF),
                pltpu.VMEM((R, D), BF),
                pltpu.VMEM((H - 1, T, D), BF),
                pltpu.VMEM((R, D), BF),
                pltpu.VMEM((R, FW), F32),
                pltpu.VMEM((R, FW), F32),
                pltpu.VMEM((R, FW), BF),
                dma((2 + 2 * CHUNKS,)),
                dma((3,)),
                dma((H - 1, 3)), dma((H - 1, 3)),
                dma((B, 2)), dma((B, 2)),
                dma((B, 2)), dma((B, 2)),
                dma((max(H - 1, 6), CHUNKS)), dma((max(H - 1, 6), CHUNKS)),
                dma((max(H - 1, 6), CHUNKS)), dma((max(H - 1, 6), CHUNKS)),
                dma((max(H - 1, 6), CHUNKS)), dma((max(H - 1, 6), CHUNKS)),
            ],
            compiler_params=pltpu.CompilerParams(
                collective_id=0, has_side_effects=True, vmem_limit_bytes=67_043_328
            ),
        )(hid, q, k, v, gain.reshape(1, -1), wo, wg, wu, wd)

    rows = P(("blk", "head"), None)
    return jax.shard_map(
        local,
        mesh=mesh,
        in_specs=(rows, rows, rows, rows, P("head", None), P(), P(None, "head"), P(None, "head"), P("head", None)),
        out_specs=rows,
        check_vma=False,
    )
```

```python
import functools

import jax
import jax.numpy as jnp
from jax import lax
from jax.experimental import pallas as pl
from jax.experimental.pallas import tpu as pltpu
from jax.sharding import PartitionSpec as P

HEADS = 16
KV_HEADS = 8
HEAD_DIM = 128
CHUNKS = 4
AHEAD = 2
SUBS = (2, 2, 2, 2)
LEAD = 3
LAG = 2
QB = 128
WIDTHS = (1, 1, 2, 2, 2)
LOG2E = 1.4426950408889634
MESH = pl.DeviceIdType.MESH
BF = jnp.bfloat16
F32 = jnp.float32


def tile_of(n, most=256):
    t = most
    while n % t:
        t -= 128
    return t


def remote(src, dst, send, recv, axis, index):
    return pltpu.make_async_remote_copy(
        src_ref=src, dst_ref=dst, send_sem=send, recv_sem=recv,
        device_id={axis: index}, device_id_type=MESH,
    )


def general_kernel(
    H, B,
    hid, q_in, k_in, v_in, gain, wo_h, wg_h, wu_h, wd_h,
    out,
    wo, wg, wu, wd, qb, kv, att, part, rs, gath, accg, accu, inner,
    w_sem, loc_sem, a_s, a_r, z_s, z_r, d_s, d_r, rs_s, rs_r, ag_s, ag_r, r2_s, r2_r,
):
    h = lax.axis_index("head")
    b = lax.axis_index("blk")
    J = B // 2
    j = b // 2
    c = b % 2
    partner = b + 1 - 2 * c
    T = hid.shape[0]
    D = hid.shape[1]
    R = T * H
    QW = qb.shape[1]
    KW = kv.shape[3]
    nh = QW // HEAD_DIM
    ratio = HEADS // KV_HEADS
    CW = D // CHUNKS
    FW = wg.shape[1]

    wcopies = [pltpu.make_async_copy(wo_h, wo, w_sem.at[0])]
    for i in range(CHUNKS):
        rows = pl.ds(i * CW, CW)
        wcopies.append(pltpu.make_async_copy(wg_h.at[rows], wg.at[rows], w_sem.at[1 + 2 * i]))
        wcopies.append(pltpu.make_async_copy(wu_h.at[rows], wu.at[rows], w_sem.at[2 + 2 * i]))
    wcopies.append(pltpu.make_async_copy(wd_h, wd, w_sem.at[1 + 2 * CHUNKS]))
    barrier = pltpu.get_barrier_semaphore()
    for d in range(1, H):
        pl.semaphore_signal(barrier, inc=1, device_id={"head": lax.rem(h + d, H)}, device_id_type=MESH)

    @pl.when(j > 0)
    def _():
        pl.semaphore_signal(barrier, inc=1, device_id={"blk": lax.rem(b + B - 2, B)}, device_id_type=MESH)

    @pl.when(j < J - 1)
    def _():
        pl.semaphore_signal(barrier, inc=1, device_id={"blk": lax.rem(b + 2, B)}, device_id_type=MESH)

    pl.semaphore_signal(barrier, inc=1, device_id={"blk": partner}, device_id_type=MESH)
    pl.semaphore_wait(barrier, H + jnp.minimum(j, 1) + jnp.minimum(J - 1 - j, 1))

    my_rows = pl.ds(pl.multiple_of(h * T, T), T)

    def cols(p, w):
        return pl.ds(pl.multiple_of(p * w, w), w)

    a_copies = []
    for t, (src, dst, w) in enumerate(
        ((k_in, kv.at[b, 0], KW), (v_in, kv.at[b, 1], KW), (q_in, qb, QW))
    ):
        for d in range(1, H):
            p = lax.rem(h + d, H)
            cp = remote(
                src.at[:, cols(p, w)], dst.at[my_rows, :],
                a_s.at[d - 1, t], a_r.at[d - 1, t], "head", p,
            )
            cp.start()
            a_copies.append((t, cp))
        lc = pltpu.make_async_copy(src.at[:, cols(h, w)], dst.at[my_rows, :], loc_sem.at[t])
        lc.start()
        a_copies.append((t, lc))

    def wait_in(t):
        for tt, cp in a_copies:
            if tt == t:
                cp.wait()

    def z_copy(slot, t):
        return remote(
            kv.at[slot, t], kv.at[slot, t], z_s.at[slot, t], z_r.at[slot, t],
            "blk", lax.rem(b + 2, B),
        )

    def d_copy(slot, t):
        return remote(
            kv.at[slot, t], kv.at[slot, t], d_s.at[slot, t], d_r.at[slot, t], "blk", partner
        )

    for t in range(2):
        wait_in(t)

        @pl.when(j < J - 1)
        def _():
            z_copy(b, t).start()

        @pl.when(c == 0)
        def _():
            d_copy(b, t).start()

    wait_in(2)
    for w in wcopies:
        w.start()

    mq = lambda n: slice(n * HEAD_DIM, (n + 1) * HEAD_DIM)
    ml = lambda n: slice((nh + n) * HEAD_DIM, (nh + n + 1) * HEAD_DIM)
    scale = HEAD_DIM ** (-0.5)

    def absorb(slot, first):
        for n in range(nh):
            g = n // ratio
            s = lax.dot_general(
                qb[:, mq(n)], kv[slot, 0, :, mq(g)],
                (((1,), (1,)), ((), ())), preferred_element_type=F32,
            ) * scale
            if first:
                qi = lax.broadcasted_iota(jnp.int32, s.shape, 0)
                ki = lax.broadcasted_iota(jnp.int32, s.shape, 1)
                s = jnp.where(ki <= qi, s, -1e30)
            top = jnp.max(s, axis=1, keepdims=True)
            if not first:
                old = accu[:, mq(n)][:, :1]
                top = jnp.maximum(top, old)
            e = jnp.exp(s - top)
            tot = jnp.sum(e, axis=1, keepdims=True)
            pv = jnp.dot(e.astype(BF), kv[slot, 1, :, mq(g)], preferred_element_type=F32)
            if not first:
                f = jnp.exp(old - top)
                tot = tot + accu[:, ml(n)][:, :1] * f
                pv = pv + accg[:, mq(n)] * f
            accu[:, mq(n)] = jnp.broadcast_to(top, (R, HEAD_DIM))
            accu[:, ml(n)] = jnp.broadcast_to(tot, (R, HEAD_DIM))
            accg[:, mq(n)] = pv

    absorb(b, True)

    @pl.when(c == 1)
    def _():
        for t in range(2):
            d_copy(b - 1, t).wait_recv()
        absorb(b - 1, False)

    def chain(s, carry):
        slot = 2 * (j - 1 - s) + c
        other = 2 * (j - 1 - s) + 1 - c
        for t in range(2):
            z_copy(slot, t).wait_recv()

            @pl.when(j < J - 1)
            def _():
                z_copy(slot, t).start()

            d_copy(slot, t).start()
        absorb(slot, False)
        for t in range(2):
            d_copy(other, t).wait_recv()
        absorb(other, False)
        return carry

    lax.fori_loop(0, j, chain, 0)

    for n in range(nh):
        att[:, mq(n)] = (accg[:, mq(n)] / accu[:, ml(n)]).astype(BF)

    square_ring = H == 4
    nx = h + 1 - 2 * (h % 2)
    ny = lax.rem(h + H // 2, H)
    dg = H - 1 - h
    HW = CW // 2

    def rows_of(p):
        return pl.ds(pl.multiple_of(p * T, T), T)

    def halves(i):
        return pl.ds(i * CW, HW), pl.ds(i * CW + HW, HW)

    def scatter(w_ref, x_ref, send, recv):
        copies = {}
        ct = tile_of(CW)
        for i in range(CHUNKS):
            def step(t, carry):
                cs = pl.ds(pl.multiple_of(i * CW + t * ct, ct), ct)
                part[:, cs] = jnp.dot(
                    x_ref[...], w_ref[:, cs], preferred_element_type=F32
                ).astype(BF)
                return carry

            lax.fori_loop(0, CW // ct, step, 0)
            if square_ring:
                ha, hb = halves(i)
                plan = ((1, dg, ha, 0, nx), (1, dg, hb, 1, ny), (0, nx, ha, 2, nx), (0, ny, hb, 3, ny))
            else:
                cs = pl.ds(i * CW, CW)
                plan = [(d - 1, lax.rem(h + d, H), cs, d - 1, lax.rem(h + d, H)) for d in range(1, H)]
            for place, block, cs, sem, to in plan:
                cp = remote(
                    part.at[rows_of(block), cs], rs.at[place, :, cs],
                    send.at[sem, i], recv.at[sem, i], "head", to,
                )
                cp.start()
                copies[sem, i] = cp
        return copies

    def combine(i, copies, send, recv):
        if not square_ring:
            return
        ha, hb = halves(i)
        for cs, sem, to in ((ha, 0, ny), (hb, 1, nx)):
            copies[sem, i].wait_recv()
            blk_rows = rows_of(to)
            part[blk_rows, cs] = (
                part[blk_rows, cs].astype(F32) + rs[1, :, cs].astype(F32)
            ).astype(BF)
            cp = remote(
                part.at[blk_rows, cs], rs.at[2, :, cs],
                send.at[4 + sem, i], recv.at[4 + sem, i], "head", to,
            )
            cp.start()
            copies[4 + sem, i] = cp

    def reduced(i, copies):
        cs = pl.ds(i * CW, CW)
        sems = (2, 3, 4, 5) if square_ring else range(H - 1)
        for sem in sems:
            copies[sem, i].wait_recv()
        total = part[my_rows, cs].astype(F32)
        for place in (0, 2) if square_ring else range(H - 1):
            total = total + rs[place, :, cs].astype(F32)
        return total

    wcopies[0].wait()
    rs_copies = scatter(wo, att, rs_s, rs_r)
    ag_copies = {}

    def spread(rows, cs, sem, i, to):
        cp = remote(
            gath.at[rows, cs], gath.at[rows, cs],
            ag_s.at[sem, i], ag_r.at[sem, i], "head", to,
        )
        cp.start()
        ag_copies[sem, i] = cp

    def spread_own(i):
        for sem, to in enumerate(
            (nx, ny) if square_ring else [lax.rem(h + d, H) for d in range(1, H)]
        ):
            spread(my_rows, pl.ds(i * CW, CW), sem, i, to)

    for i in range(CHUNKS + 1):
        if i < CHUNKS:
            combine(i, rs_copies, rs_s, rs_r)
        if i:
            cs = pl.ds((i - 1) * CW, CW)
            gath[my_rows, cs] = (hid[:, cs].astype(F32) + reduced(i - 1, rs_copies)).astype(BF)
            if i <= AHEAD or not square_ring:
                spread_own(i - 1)

    ft = tile_of(FW)
    square = jnp.zeros((R, 1), F32)
    for i in range(CHUNKS + 1):
        if i < CHUNKS and square_ring:
            ha, hb = halves(i)
            ag_copies[0, i].wait_recv()
            spread(rows_of(nx), ha, 2, i, ny)
            ag_copies[1, i].wait_recv()
            spread(rows_of(ny), hb, 3, i, nx)
            if i + AHEAD < CHUNKS:
                spread_own(i + AHEAD)
        if i == 0:
            continue
        k = i - 1
        cs = pl.ds(k * CW, CW)
        for sem in (2, 3) if square_ring else range(H - 1):
            ag_copies[sem, k].wait_recv()
        wcopies[1 + 2 * k].wait()
        wcopies[2 + 2 * k].wait()
        x = gath[:, cs].astype(F32)
        square = square + jnp.sum(x * x, axis=1, keepdims=True)
        xg = (x * gain[:, cs]).astype(BF)

        def step(t, carry, xg=xg, cs=cs, k=k):
            fs = pl.ds(pl.multiple_of(t * ft, ft), ft)
            g = jnp.dot(xg, wg[cs, fs], preferred_element_type=F32)
            u = jnp.dot(xg, wu[cs, fs], preferred_element_type=F32)
            if k:
                g = g + accg[:, fs]
                u = u + accu[:, fs]
            accg[:, fs] = g
            accu[:, fs] = u
            return carry

        lax.fori_loop(0, FW // ft, step, 0)
    r = lax.rsqrt(square / D + 1e-5)

    def act(t, carry):
        fs = pl.ds(pl.multiple_of(t * ft, ft), ft)
        g = accg[:, fs] * r
        u = accu[:, fs] * r
        inner[:, fs] = (g / (1.0 + jnp.exp(-g)) * u).astype(BF)
        return carry

    lax.fori_loop(0, FW // ft, act, 0)
    for cp in rs_copies.values():
        cp.wait_send()
    wcopies[-1].wait()
    r2_copies = scatter(wd, inner, r2_s, r2_r)
    for i in range(CHUNKS + 1):
        if i < CHUNKS:
            combine(i, r2_copies, r2_s, r2_r)
        if i:
            cs = pl.ds((i - 1) * CW, CW)
            out[:, cs] = (gath[my_rows, cs].astype(F32) + reduced(i - 1, r2_copies)).astype(BF)

    for cp in (*ag_copies.values(), *r2_copies.values()):
        cp.wait_send()
    for t in range(2):
        @pl.when(j < J - 1)
        def _():
            z_copy(b, t).wait_send()

        @pl.when(c == 0)
        def _():
            d_copy(b, t).wait_send()

    def drain(s, carry):
        slot = 2 * (j - 1 - s) + c
        for t in range(2):
            @pl.when(j < J - 1)
            def _():
                z_copy(slot, t).wait_send()

            d_copy(slot, t).wait_send()
        return carry

    lax.fori_loop(0, j, drain, 0)


def square_kernel(
    H, B,
    hid_h, q_h, k_h, v_h, gain, wo_h, wg_h, wu_h, wd_h,
    out,
    hid, q_in, k_in, v_in, wo, wg, wu, wd, qb, kv, att, attx, hx, sb, rb, part, rs, gath, accg, accu, inner,
    i_sem, w_sem, a_s, a_r, z_s, z_r, d_s, d_r, x_s, x_r, at_s, at_r, o_s, o_r, ag_s, ag_r, r2_s, r2_r,
):
    h = lax.axis_index("head")
    b = lax.axis_index("blk")
    J = B // 2
    j = b // 2
    c = b % 2
    partner = b + 1 - 2 * c
    T, D = hid.shape
    R = T * H
    G = kv.shape[1]
    QW = qb.shape[1]
    ratio = QW // G // HEAD_DIM
    GW = QW // G
    FW = wg.shape[1]
    half = D // 2
    DW = D // 4
    grain = DW // sum(SUBS)
    subs = [(sum(SUBS[:i]) * grain, w * grain) for i, w in enumerate(SUBS)]

    ex, ey = h % 2, h // 2
    nx = h + 1 - 2 * ex
    ny = lax.rem(h + 2, H)
    dg = H - 1 - h
    pair = (nx, ny)
    across = (ny, nx)
    mine = (ex, ey)

    wcopies = []
    for s in range(2):
        src = wo_h.at[:, pl.ds(pl.multiple_of(s * half + mine[s] * DW, DW), DW)]
        wcopies.append((src, wo.at[s, pl.ds(0, QW)]))
    for i in range(CHUNKS):
        rows = pl.ds(i * (D // CHUNKS), D // CHUNKS)
        wcopies.append((wg_h.at[rows], wg.at[rows]))
        wcopies.append((wu_h.at[rows], wu.at[rows]))
    wcopies.append((wd_h, wd))
    wcopies = [pltpu.make_async_copy(s, d, w_sem.at[n]) for n, (s, d) in enumerate(wcopies)]

    staged = [
        pltpu.make_async_copy(src, dst, i_sem.at[n])
        for n, (src, dst) in enumerate(((k_h, k_in), (v_h, v_in), (q_h, q_in), (hid_h, hid)))
    ]
    for cp in staged:
        cp.start()
    barrier = pltpu.get_barrier_semaphore()
    for d in range(1, H):
        pl.semaphore_signal(barrier, inc=1, device_id={"head": lax.rem(h + d, H)}, device_id_type=MESH)

    @pl.when(j > 0)
    def _():
        pl.semaphore_signal(barrier, inc=1, device_id={"blk": lax.rem(b + B - 2, B)}, device_id_type=MESH)

    @pl.when(j < J - 1)
    def _():
        pl.semaphore_signal(barrier, inc=1, device_id={"blk": lax.rem(b + 2, B)}, device_id_type=MESH)

    pl.semaphore_signal(barrier, inc=1, device_id={"blk": partner}, device_id_type=MESH)
    pl.semaphore_wait(barrier, H + jnp.minimum(j, 1) + jnp.minimum(J - 1 - j, 1))

    for cp in staged[:2]:
        cp.wait()

    def rows_of(p):
        return pl.ds(pl.multiple_of(p * T, T), T)

    my_rows = rows_of(h)

    pieces = []
    for g in range(G):
        pieces.append((k_in, G, g, kv.at[b, g, 0, my_rows, :]))
        pieces.append((v_in, G, g, kv.at[b, g, 1, my_rows, :]))
    pieces.append((q_in, 1, 0, qb.at[my_rows, :]))

    def piece_cols(p, per, n, dst):
        w = dst.shape[1]
        return pl.ds(pl.multiple_of((p * per + n) * w, w), w)

    a_copies = []
    for t, (src, per, n, dst) in enumerate(pieces):
        if src is q_in:
            staged[2].wait()
        cps = []
        for d, p in enumerate((dg, nx, ny)):
            cp = remote(src.at[:, piece_cols(p, per, n, dst)], dst, a_s.at[d, t], a_r.at[d, t], "head", p)
            cp.start()
            cps.append(cp)
        a_copies.append(cps)

    x_copies = []
    for s in range(2):
        cs = pl.ds(pl.multiple_of(s * half + (1 - mine[s]) * DW, DW), DW)
        x_copies.append(remote(hid.at[:, cs], hx.at[s], x_s.at[s], x_r.at[s], "head", pair[s]))
    core_cols = pl.ds(pl.multiple_of(c * (DW // 2), DW // 2), DW // 2)
    for s in range(2):
        cs = pl.ds(pl.multiple_of(s * half + (1 - mine[s]) * DW + c * (DW // 2), DW // 2), DW // 2)
        x_copies.append(remote(
            wo_h.at[:, cs], wo.at[s, pl.ds(QW, QW), core_cols],
            x_s.at[2 + s], x_r.at[2 + s], "head", pair[s],
        ))
    staged[3].wait()
    for cp in x_copies:
        cp.start()
    share = []
    for s in range(2):
        ref = wo.at[s, pl.ds(QW, QW), core_cols]
        share.append(remote(ref, ref, x_s.at[4 + s], x_r.at[4 + s], "blk", partner))

    for t, (src, per, n, dst) in enumerate(pieces):
        dst[...] = src[:, piece_cols(h, per, n, dst)]

    def wait_in(t):
        for cp in a_copies[t]:
            cp.wait_recv()

    def z_copy(slot, g, t):
        ref = kv.at[slot, g, t]
        return remote(ref, ref, z_s.at[slot, g, t], z_r.at[slot, g, t], "blk", lax.rem(b + 2, B))

    def d_copy(slot, g, t):
        ref = kv.at[slot, g, t]
        return remote(ref, ref, d_s.at[slot, g, t], d_r.at[slot, g, t], "blk", partner)

    own = [(g, t) for g in range(G) for t in range(2)]
    for n, (g, t) in enumerate(own):
        wait_in(n)

        @pl.when((j < J - 1) & ((j == 0) | (n < len(own) - 1)))
        def _():
            z_copy(b, g, t).start()

        @pl.when(c == 0)
        def _():
            d_copy(b, g, t).start()

    def pass_on(slot, g, t):
        z_copy(slot, g, t).wait_recv()

        @pl.when(j < J - 1)
        def _():
            z_copy(slot, g, t).start()

        d_copy(slot, g, t).start()

    def both(s):
        first = 2 * (j - 1 - s)
        return first + c, first + 1 - c

    def pass_on_first(g):
        @pl.when(j > 0)
        def _():
            for t in range(2):
                pass_on(both(0)[0], g, t)

    pass_on_first(0)

    @pl.when((j > 0) & (j < J - 1))
    def _():
        z_copy(b, *own[-1]).start()

    wait_in(len(own))
    for w in wcopies:
        w.start()

    factor = HEAD_DIM ** (-0.5) * LOG2E

    def absorb(g, slots, first):
        ones = jnp.ones((R, HEAD_DIM), BF)
        keys = jnp.concatenate([kv[slot, g, 0] for slot in slots], axis=0)
        values = jnp.concatenate(
            [jnp.concatenate([kv[slot, g, 1], ones], axis=1) for slot in slots], axis=0
        )
        for r in range(ratio):
            n = g * ratio + r
            tops = slice(n * HEAD_DIM, (n + 1) * HEAD_DIM)
            sums = slice(2 * n * HEAD_DIM, 2 * (n + 1) * HEAD_DIM)
            for q0 in range(0, R, QB):
                rows = slice(q0, q0 + QB)
                sc = lax.dot_general(
                    qb[rows, tops], keys,
                    (((1,), (1,)), ((), ())), preferred_element_type=F32,
                )
                tiles = [sc[:, t:t + HEAD_DIM] for t in range(0, len(slots) * R, HEAD_DIM)]
                if first:
                    qi = q0 + lax.broadcasted_iota(jnp.int32, tiles[0].shape, 0)
                    ki = lax.broadcasted_iota(jnp.int32, tiles[0].shape, 1)
                    for t in range(R // HEAD_DIM):
                        tiles[t] = jnp.where(ki + t * HEAD_DIM <= qi, tiles[t], -1e30)
                top = functools.reduce(jnp.maximum, tiles)
                top = jnp.broadcast_to(jnp.max(top, axis=1, keepdims=True), top.shape)
                if not first:
                    old = accu[rows, tops]
                    top = jnp.maximum(top, old)
                peak = top * factor
                e = jnp.concatenate([jnp.exp2(t * factor - peak).astype(BF) for t in tiles], axis=1)
                pv = jnp.dot(e, values, preferred_element_type=F32)
                if not first:
                    f = jnp.exp2(old * factor - peak)
                    pv = pv + accg[rows, sums] * jnp.concatenate([f, f], axis=1)
                accu[rows, tops] = top
                accg[rows, sums] = pv

    for g in range(G):
        @pl.when(c == 0)
        def _(g=g):
            absorb(g, (b,), True)

        @pl.when(c == 1)
        def _(g=g):
            for t in range(2):
                d_copy(b - 1, g, t).wait_recv()
            absorb(g, (b, b - 1), True)

    at_copies = []
    for g in range(G):
        def chain(s, carry, g=g):
            slot, other = both(s)

            @pl.when(s > 0)
            def _():
                for t in range(2):
                    pass_on(slot, g, t)

            for t in range(2):
                d_copy(other, g, t).wait_recv()
            absorb(g, (slot, other), False)
            return carry

        lax.fori_loop(0, j, chain, 0)
        if g + 1 < G:
            pass_on_first(g + 1)
        for r in range(ratio):
            n = g * ratio + r
            pv = accg[:, 2 * n * HEAD_DIM:2 * (n + 1) * HEAD_DIM]
            att[:, n * HEAD_DIM:(n + 1) * HEAD_DIM] = (pv[:, :HEAD_DIM] / pv[:, HEAD_DIM:]).astype(BF)
        cs = pl.ds(g * GW, GW)
        for s in range(2):
            cp = remote(att.at[:, cs], attx.at[s, :, cs], at_s.at[g, s], at_r.at[g, s], "head", pair[s])
            cp.start()
            at_copies.append(cp)

    accs = (accg, accu)
    for s in range(2):
        x_copies[2 + s].wait_recv()
        share[s].start()
    for s in range(2):
        wcopies[s].wait()
        for t in range(0, DW, tile_of(DW)):
            cs = slice(t, t + tile_of(DW))
            accs[s][:, cs] = jnp.dot(att[...], wo[s, :QW, cs], preferred_element_type=F32)
    for s in range(2):
        share[s].wait_recv()
    for cp in at_copies:
        cp.wait_recv()

    co = ({"h": nx, "x": h, "y": dg, "d": ny}, {"h": ny, "x": dg, "y": h, "d": nx})
    order = [(s, i) for i in range(len(subs)) for s in range(2)]
    o_copies = {}
    for s, i in order:
        cs = pl.ds(*subs[i])
        accs[s][:, cs] += jnp.dot(attx[s], wo[s, QW:, cs], preferred_element_type=F32)
        to = across[s]
        away = (to, co[s]["y" if s == 0 else "x"])
        for n, p in enumerate(away):
            sb[s, n * T:(n + 1) * T, cs] = accs[s][rows_of(p), cs].astype(BF)
        cp = remote(sb.at[s, :, cs], rb.at[s, :, cs], o_s.at[s, i], o_r.at[s, i], "head", to)
        cp.start()
        o_copies[s, i] = cp

    def cols_of(s, i, other):
        part_index = 1 - mine[s] if other else mine[s]
        at, w = subs[i]
        return pl.ds(pl.multiple_of(s * half + part_index * DW + at, grain), w)

    ag_copies = {}

    def spread(s, i, kind, rows, cs, to):
        ref = gath.at[rows, cs]
        cp = remote(ref, ref, ag_s.at[s, i, kind], ag_r.at[s, i, kind], "head", to)
        cp.start()
        ag_copies[s, i, kind] = cp

    def spread_own(s, i):
        cs = cols_of(s, i, False)
        for n, to in enumerate((nx, ny)):
            spread(s, i, 2 * n, my_rows, cs, to)
            spread(s, i, 2 * n + 1, rows_of(co[s]["h"]), cs, to)

    def relay(s, i):
        ag_copies[s, i, 0].wait_recv()
        spread(s, i, 4, rows_of(nx), cols_of(s, i, s == 0), ny)
        ag_copies[s, i, 3].wait_recv()
        spread(s, i, 5, rows_of(co[s]["y"]), cols_of(s, i, s == 1), nx)

    for s in range(2):
        x_copies[s].wait_recv()
    for k, (s, i) in enumerate(order):
        o_copies[s, i].wait_recv()
        cs = cols_of(s, i, False)
        lc = pl.ds(*subs[i])
        gath[my_rows, cs] = (
            hid[:, cs].astype(F32) + (accs[s][my_rows, lc] + rb[s, :T, lc].astype(F32))
        ).astype(BF)
        cr = rows_of(co[s]["h"])
        gath[cr, cs] = (
            hx[s, :, lc].astype(F32) + (accs[s][cr, lc] + rb[s, T:, lc].astype(F32))
        ).astype(BF)
        if k < LEAD:
            spread_own(s, i)

    for w in wcopies[2:-1]:
        w.wait()
    ft = tile_of(FW)
    square = jnp.zeros((R, 1), F32)
    for n in range(len(order) + LAG):
        if n < len(order):
            relay(*order[n])
            if n + LEAD < len(order):
                spread_own(*order[n + LEAD])
        if n < LAG:
            continue
        k = n - LAG
        s, i = order[k]
        for kind in (1, 2, 4, 5):
            ag_copies[s, i, kind].wait_recv()
        start, SW = subs[i]
        at = (s * half + start, s * half + DW + start)
        xs = []
        for a in at:
            x = gath[:, a:a + SW].astype(F32)
            square = square + jnp.sum(x * x, axis=1, keepdims=True)
            xs.append((x * gain[:, a:a + SW]).astype(BF))

        last = k == len(order) - 1
        if last:
            r = lax.rsqrt(square / D + 1e-5)
        for t in range(FW // ft):
            fs = slice(t * ft, (t + 1) * ft)
            ys = []
            for acc, w in ((accg, wg), (accu, wu)):
                y = jnp.dot(xs[0], w[at[0]:at[0] + SW, fs], preferred_element_type=F32)
                y = y + jnp.dot(xs[1], w[at[1]:at[1] + SW, fs], preferred_element_type=F32)
                if k:
                    y = y + acc[:, fs]
                if last:
                    ys.append(y * r)
                else:
                    acc[:, fs] = y
            if last:
                g, u = ys
                inner[:, fs] = (g / (1.0 + jnp.exp(-g)) * u).astype(BF)
    wcopies[-1].wait()

    unit = D // sum(WIDTHS)
    spans = [(sum(WIDTHS[:i]) * unit, w * unit) for i, w in enumerate(WIDTHS)]

    def halves(i):
        at, w = spans[i]
        return pl.ds(at, w // 2), pl.ds(at + w // 2, w // 2)

    copies = {}

    def send(i, sem, rows, place, cs, to):
        cp = remote(part.at[rows, cs], rs.at[place, :, cs], r2_s.at[sem, i], r2_r.at[sem, i], "head", to)
        cp.start()
        copies[sem, i] = cp

    for i, (at, w) in enumerate(spans):
        ct = tile_of(w)
        for t in range(w // ct):
            cs = slice(at + t * ct, at + (t + 1) * ct)
            part[:, cs] = jnp.dot(inner[...], wd[:, cs], preferred_element_type=F32).astype(BF)
        ha, hb = halves(i)
        send(i, 0, rows_of(dg), 1, ha, nx)
        send(i, 1, rows_of(dg), 1, hb, ny)
        send(i, 2, rows_of(nx), 0, ha, nx)
        send(i, 3, rows_of(ny), 0, hb, ny)
    for i in range(len(spans)):
        ha, hb = halves(i)
        for cs, sem, to in ((ha, 0, ny), (hb, 1, nx)):
            copies[sem, i].wait_recv()
            rows = rows_of(to)
            part[rows, cs] = (part[rows, cs].astype(F32) + rs[1, :, cs].astype(F32)).astype(BF)
            send(i, 4 + sem, rows, 2, cs, to)
    for i in range(len(spans)):
        cs = pl.ds(*spans[i])
        for sem in (2, 3, 4, 5):
            copies[sem, i].wait_recv()
        total = part[my_rows, cs].astype(F32)
        for place in (0, 2):
            total = total + rs[place, :, cs].astype(F32)
        out[:, cs] = (gath[my_rows, cs].astype(F32) + total).astype(BF)

    for cps in a_copies:
        for cp in cps:
            cp.wait_send()
    for cp in (*x_copies, *share, *at_copies, *o_copies.values(), *ag_copies.values(), *copies.values()):
        cp.wait_send()
    for g, t in own:
        @pl.when(j < J - 1)
        def _():
            z_copy(b, g, t).wait_send()

        @pl.when(c == 0)
        def _():
            d_copy(b, g, t).wait_send()

    def drain(s, carry):
        slot = 2 * (j - 1 - s) + c
        for g, t in own:
            @pl.when(j < J - 1)
            def _():
                z_copy(slot, g, t).wait_send()

            d_copy(slot, g, t).wait_send()
        return carry

    lax.fori_loop(0, j, drain, 0)


def square_call(H, B, hid, q, k, v, wo, gain, wg, wu, wd):
    T, D = hid.shape
    R = T * H
    QW = q.shape[1] // H
    G = k.shape[1] // H // HEAD_DIM
    FW = wg.shape[1]
    ratio = QW // HEAD_DIM // G
    AW = max(FW, D // 4, 2 * QW)
    vm = pl.BlockSpec(memory_space=pltpu.VMEM)
    hbm = pl.BlockSpec(memory_space=pl.ANY)
    dma = pltpu.SemaphoreType.DMA
    return pl.pallas_call(
        functools.partial(square_kernel, H, B),
        out_shape=pltpu.VMEM((T, D), BF),
        in_specs=[hbm] * 4 + [vm] + [hbm] * 4,
        out_specs=vm,
        scratch_shapes=[
            pltpu.VMEM(hid.shape, BF),
            pltpu.VMEM(q.shape, BF),
            pltpu.VMEM(k.shape, BF),
            pltpu.VMEM(v.shape, BF),
            pltpu.VMEM((2, 2 * QW, D // 4), BF),
            pltpu.VMEM(wg.shape, BF),
            pltpu.VMEM(wu.shape, BF),
            pltpu.VMEM(wd.shape, BF),
            pltpu.VMEM((R, QW), BF),
            pltpu.VMEM((B, G, 2, R, HEAD_DIM), BF),
            pltpu.VMEM((R, QW), BF),
            pltpu.VMEM((2, R, QW), BF),
            pltpu.VMEM((2, T, D // 4), BF),
            pltpu.VMEM((2, 2 * T, D // 4), BF),
            pltpu.VMEM((2, 2 * T, D // 4), BF),
            pltpu.VMEM((R, D), BF),
            pltpu.VMEM((3, T, D), BF),
            pltpu.VMEM((R, D), BF),
            pltpu.VMEM((R, AW), F32),
            pltpu.VMEM((R, AW), F32),
            pltpu.VMEM((R, FW), BF),
            dma((4,)),
            dma((3 + 2 * CHUNKS,)),
            dma((H - 1, 2 * G + 1)), dma((H - 1, 2 * G + 1)),
            dma((B, G, 2)), dma((B, G, 2)),
            dma((B, G, 2)), dma((B, G, 2)),
            dma((6,)), dma((6,)),
            dma((G, 2)), dma((G, 2)),
            dma((2, len(SUBS))), dma((2, len(SUBS))),
            dma((2, len(SUBS), 6)), dma((2, len(SUBS), 6)),
            dma((6, len(WIDTHS))), dma((6, len(WIDTHS))),
        ],
        compiler_params=pltpu.CompilerParams(
            collective_id=0, has_side_effects=True, vmem_limit_bytes=66_400_000
        ),
    )(hid, q, k, v, gain.reshape(1, -1), wo, wg, wu, wd)


def solution(mesh):
    H = mesh.shape["head"]
    B = mesh.shape["blk"]

    def local(hid, q, k, v, wo, gain, wg, wu, wd):
        if H == 4:
            return square_call(H, B, hid, q, k, v, wo, gain, wg, wu, wd)
        T, D = hid.shape
        R = T * H
        QW = q.shape[1] // H
        KW = k.shape[1] // H
        FW = wg.shape[1]
        vm = pl.BlockSpec(memory_space=pltpu.VMEM)
        hbm = pl.BlockSpec(memory_space=pl.ANY)
        dma = pltpu.SemaphoreType.DMA
        return pl.pallas_call(
            functools.partial(general_kernel, H, B),
            out_shape=jax.ShapeDtypeStruct((T, D), BF),
            in_specs=[vm] * 5 + [hbm] * 4,
            out_specs=vm,
            scratch_shapes=[
                pltpu.VMEM(wo.shape, BF),
                pltpu.VMEM(wg.shape, BF),
                pltpu.VMEM(wu.shape, BF),
                pltpu.VMEM(wd.shape, BF),
                pltpu.VMEM((R, QW), BF),
                pltpu.VMEM((B, 2, R, KW), BF),
                pltpu.VMEM((R, QW), BF),
                pltpu.VMEM((R, D), BF),
                pltpu.VMEM((H - 1, T, D), BF),
                pltpu.VMEM((R, D), BF),
                pltpu.VMEM((R, FW), F32),
                pltpu.VMEM((R, FW), F32),
                pltpu.VMEM((R, FW), BF),
                dma((2 + 2 * CHUNKS,)),
                dma((3,)),
                dma((H - 1, 3)), dma((H - 1, 3)),
                dma((B, 2)), dma((B, 2)),
                dma((B, 2)), dma((B, 2)),
                dma((max(H - 1, 6), CHUNKS)), dma((max(H - 1, 6), CHUNKS)),
                dma((max(H - 1, 6), CHUNKS)), dma((max(H - 1, 6), CHUNKS)),
                dma((max(H - 1, 6), CHUNKS)), dma((max(H - 1, 6), CHUNKS)),
            ],
            compiler_params=pltpu.CompilerParams(
                collective_id=0, has_side_effects=True, vmem_limit_bytes=67_043_328
            ),
        )(hid, q, k, v, gain.reshape(1, -1), wo, wg, wu, wd)

    rows = P(("blk", "head"), None)
    return jax.shard_map(
        local,
        mesh=mesh,
        in_specs=(rows, rows, rows, rows, P("head", None), P(), P(None, "head"), P(None, "head"), P("head", None)),
        out_specs=rows,
        check_vma=False,
    )
```

```python
import functools

import jax
import jax.numpy as jnp
from jax import lax
from jax.experimental import pallas as pl
from jax.experimental.pallas import tpu as pltpu
from jax.sharding import PartitionSpec as P

HEADS = 16
KV_HEADS = 8
HEAD_DIM = 128
CHUNKS = 4
AHEAD = 2
SUBS = (2, 2, 2, 2)
LEAD = 3
LAG = 2
QB = 128
WIDTHS = (1, 1, 2, 2, 2)
LOG2E = 1.4426950408889634
MESH = pl.DeviceIdType.MESH
BF = jnp.bfloat16
F32 = jnp.float32


def tile_of(n, most=256):
    t = most
    while n % t:
        t -= 128
    return t


def remote(src, dst, send, recv, axis, index):
    return pltpu.make_async_remote_copy(
        src_ref=src, dst_ref=dst, send_sem=send, recv_sem=recv,
        device_id={axis: index}, device_id_type=MESH,
    )


def general_kernel(
    H, B,
    hid, q_in, k_in, v_in, gain, wo_h, wg_h, wu_h, wd_h,
    out,
    wo, wg, wu, wd, qb, kv, att, part, rs, gath, accg, accu, inner,
    w_sem, loc_sem, a_s, a_r, z_s, z_r, d_s, d_r, rs_s, rs_r, ag_s, ag_r, r2_s, r2_r,
):
    h = lax.axis_index("head")
    b = lax.axis_index("blk")
    J = B // 2
    j = b // 2
    c = b % 2
    partner = b + 1 - 2 * c
    T = hid.shape[0]
    D = hid.shape[1]
    R = T * H
    QW = qb.shape[1]
    KW = kv.shape[3]
    nh = QW // HEAD_DIM
    ratio = HEADS // KV_HEADS
    CW = D // CHUNKS
    FW = wg.shape[1]

    wcopies = [pltpu.make_async_copy(wo_h, wo, w_sem.at[0])]
    for i in range(CHUNKS):
        rows = pl.ds(i * CW, CW)
        wcopies.append(pltpu.make_async_copy(wg_h.at[rows], wg.at[rows], w_sem.at[1 + 2 * i]))
        wcopies.append(pltpu.make_async_copy(wu_h.at[rows], wu.at[rows], w_sem.at[2 + 2 * i]))
    wcopies.append(pltpu.make_async_copy(wd_h, wd, w_sem.at[1 + 2 * CHUNKS]))
    barrier = pltpu.get_barrier_semaphore()
    for d in range(1, H):
        pl.semaphore_signal(barrier, inc=1, device_id={"head": lax.rem(h + d, H)}, device_id_type=MESH)

    @pl.when(j > 0)
    def _():
        pl.semaphore_signal(barrier, inc=1, device_id={"blk": lax.rem(b + B - 2, B)}, device_id_type=MESH)

    @pl.when(j < J - 1)
    def _():
        pl.semaphore_signal(barrier, inc=1, device_id={"blk": lax.rem(b + 2, B)}, device_id_type=MESH)

    pl.semaphore_signal(barrier, inc=1, device_id={"blk": partner}, device_id_type=MESH)
    pl.semaphore_wait(barrier, H + jnp.minimum(j, 1) + jnp.minimum(J - 1 - j, 1))

    my_rows = pl.ds(pl.multiple_of(h * T, T), T)

    def cols(p, w):
        return pl.ds(pl.multiple_of(p * w, w), w)

    a_copies = []
    for t, (src, dst, w) in enumerate(
        ((k_in, kv.at[b, 0], KW), (v_in, kv.at[b, 1], KW), (q_in, qb, QW))
    ):
        for d in range(1, H):
            p = lax.rem(h + d, H)
            cp = remote(
                src.at[:, cols(p, w)], dst.at[my_rows, :],
                a_s.at[d - 1, t], a_r.at[d - 1, t], "head", p,
            )
            cp.start()
            a_copies.append((t, cp))
        lc = pltpu.make_async_copy(src.at[:, cols(h, w)], dst.at[my_rows, :], loc_sem.at[t])
        lc.start()
        a_copies.append((t, lc))

    def wait_in(t):
        for tt, cp in a_copies:
            if tt == t:
                cp.wait()

    def z_copy(slot, t):
        return remote(
            kv.at[slot, t], kv.at[slot, t], z_s.at[slot, t], z_r.at[slot, t],
            "blk", lax.rem(b + 2, B),
        )

    def d_copy(slot, t):
        return remote(
            kv.at[slot, t], kv.at[slot, t], d_s.at[slot, t], d_r.at[slot, t], "blk", partner
        )

    for t in range(2):
        wait_in(t)

        @pl.when(j < J - 1)
        def _():
            z_copy(b, t).start()

        @pl.when(c == 0)
        def _():
            d_copy(b, t).start()

    wait_in(2)
    for w in wcopies:
        w.start()

    mq = lambda n: slice(n * HEAD_DIM, (n + 1) * HEAD_DIM)
    ml = lambda n: slice((nh + n) * HEAD_DIM, (nh + n + 1) * HEAD_DIM)
    scale = HEAD_DIM ** (-0.5)

    def absorb(slot, first):
        for n in range(nh):
            g = n // ratio
            s = lax.dot_general(
                qb[:, mq(n)], kv[slot, 0, :, mq(g)],
                (((1,), (1,)), ((), ())), preferred_element_type=F32,
            ) * scale
            if first:
                qi = lax.broadcasted_iota(jnp.int32, s.shape, 0)
                ki = lax.broadcasted_iota(jnp.int32, s.shape, 1)
                s = jnp.where(ki <= qi, s, -1e30)
            top = jnp.max(s, axis=1, keepdims=True)
            if not first:
                old = accu[:, mq(n)][:, :1]
                top = jnp.maximum(top, old)
            e = jnp.exp(s - top)
            tot = jnp.sum(e, axis=1, keepdims=True)
            pv = jnp.dot(e.astype(BF), kv[slot, 1, :, mq(g)], preferred_element_type=F32)
            if not first:
                f = jnp.exp(old - top)
                tot = tot + accu[:, ml(n)][:, :1] * f
                pv = pv + accg[:, mq(n)] * f
            accu[:, mq(n)] = jnp.broadcast_to(top, (R, HEAD_DIM))
            accu[:, ml(n)] = jnp.broadcast_to(tot, (R, HEAD_DIM))
            accg[:, mq(n)] = pv

    absorb(b, True)

    @pl.when(c == 1)
    def _():
        for t in range(2):
            d_copy(b - 1, t).wait_recv()
        absorb(b - 1, False)

    def chain(s, carry):
        slot = 2 * (j - 1 - s) + c
        other = 2 * (j - 1 - s) + 1 - c
        for t in range(2):
            z_copy(slot, t).wait_recv()

            @pl.when(j < J - 1)
            def _():
                z_copy(slot, t).start()

            d_copy(slot, t).start()
        absorb(slot, False)
        for t in range(2):
            d_copy(other, t).wait_recv()
        absorb(other, False)
        return carry

    lax.fori_loop(0, j, chain, 0)

    for n in range(nh):
        att[:, mq(n)] = (accg[:, mq(n)] / accu[:, ml(n)]).astype(BF)

    square_ring = H == 4
    nx = h + 1 - 2 * (h % 2)
    ny = lax.rem(h + H // 2, H)
    dg = H - 1 - h
    HW = CW // 2

    def rows_of(p):
        return pl.ds(pl.multiple_of(p * T, T), T)

    def halves(i):
        return pl.ds(i * CW, HW), pl.ds(i * CW + HW, HW)

    def scatter(w_ref, x_ref, send, recv):
        copies = {}
        ct = tile_of(CW)
        for i in range(CHUNKS):
            def step(t, carry):
                cs = pl.ds(pl.multiple_of(i * CW + t * ct, ct), ct)
                part[:, cs] = jnp.dot(
                    x_ref[...], w_ref[:, cs], preferred_element_type=F32
                ).astype(BF)
                return carry

            lax.fori_loop(0, CW // ct, step, 0)
            if square_ring:
                ha, hb = halves(i)
                plan = ((1, dg, ha, 0, nx), (1, dg, hb, 1, ny), (0, nx, ha, 2, nx), (0, ny, hb, 3, ny))
            else:
                cs = pl.ds(i * CW, CW)
                plan = [(d - 1, lax.rem(h + d, H), cs, d - 1, lax.rem(h + d, H)) for d in range(1, H)]
            for place, block, cs, sem, to in plan:
                cp = remote(
                    part.at[rows_of(block), cs], rs.at[place, :, cs],
                    send.at[sem, i], recv.at[sem, i], "head", to,
                )
                cp.start()
                copies[sem, i] = cp
        return copies

    def combine(i, copies, send, recv):
        if not square_ring:
            return
        ha, hb = halves(i)
        for cs, sem, to in ((ha, 0, ny), (hb, 1, nx)):
            copies[sem, i].wait_recv()
            blk_rows = rows_of(to)
            part[blk_rows, cs] = (
                part[blk_rows, cs].astype(F32) + rs[1, :, cs].astype(F32)
            ).astype(BF)
            cp = remote(
                part.at[blk_rows, cs], rs.at[2, :, cs],
                send.at[4 + sem, i], recv.at[4 + sem, i], "head", to,
            )
            cp.start()
            copies[4 + sem, i] = cp

    def reduced(i, copies):
        cs = pl.ds(i * CW, CW)
        sems = (2, 3, 4, 5) if square_ring else range(H - 1)
        for sem in sems:
            copies[sem, i].wait_recv()
        total = part[my_rows, cs].astype(F32)
        for place in (0, 2) if square_ring else range(H - 1):
            total = total + rs[place, :, cs].astype(F32)
        return total

    wcopies[0].wait()
    rs_copies = scatter(wo, att, rs_s, rs_r)
    ag_copies = {}

    def spread(rows, cs, sem, i, to):
        cp = remote(
            gath.at[rows, cs], gath.at[rows, cs],
            ag_s.at[sem, i], ag_r.at[sem, i], "head", to,
        )
        cp.start()
        ag_copies[sem, i] = cp

    def spread_own(i):
        for sem, to in enumerate(
            (nx, ny) if square_ring else [lax.rem(h + d, H) for d in range(1, H)]
        ):
            spread(my_rows, pl.ds(i * CW, CW), sem, i, to)

    for i in range(CHUNKS + 1):
        if i < CHUNKS:
            combine(i, rs_copies, rs_s, rs_r)
        if i:
            cs = pl.ds((i - 1) * CW, CW)
            gath[my_rows, cs] = (hid[:, cs].astype(F32) + reduced(i - 1, rs_copies)).astype(BF)
            if i <= AHEAD or not square_ring:
                spread_own(i - 1)

    ft = tile_of(FW)
    square = jnp.zeros((R, 1), F32)
    for i in range(CHUNKS + 1):
        if i < CHUNKS and square_ring:
            ha, hb = halves(i)
            ag_copies[0, i].wait_recv()
            spread(rows_of(nx), ha, 2, i, ny)
            ag_copies[1, i].wait_recv()
            spread(rows_of(ny), hb, 3, i, nx)
            if i + AHEAD < CHUNKS:
                spread_own(i + AHEAD)
        if i == 0:
            continue
        k = i - 1
        cs = pl.ds(k * CW, CW)
        for sem in (2, 3) if square_ring else range(H - 1):
            ag_copies[sem, k].wait_recv()
        wcopies[1 + 2 * k].wait()
        wcopies[2 + 2 * k].wait()
        x = gath[:, cs].astype(F32)
        square = square + jnp.sum(x * x, axis=1, keepdims=True)
        xg = (x * gain[:, cs]).astype(BF)

        def step(t, carry, xg=xg, cs=cs, k=k):
            fs = pl.ds(pl.multiple_of(t * ft, ft), ft)
            g = jnp.dot(xg, wg[cs, fs], preferred_element_type=F32)
            u = jnp.dot(xg, wu[cs, fs], preferred_element_type=F32)
            if k:
                g = g + accg[:, fs]
                u = u + accu[:, fs]
            accg[:, fs] = g
            accu[:, fs] = u
            return carry

        lax.fori_loop(0, FW // ft, step, 0)
    r = lax.rsqrt(square / D + 1e-5)

    def act(t, carry):
        fs = pl.ds(pl.multiple_of(t * ft, ft), ft)
        g = accg[:, fs] * r
        u = accu[:, fs] * r
        inner[:, fs] = (g / (1.0 + jnp.exp(-g)) * u).astype(BF)
        return carry

    lax.fori_loop(0, FW // ft, act, 0)
    for cp in rs_copies.values():
        cp.wait_send()
    wcopies[-1].wait()
    r2_copies = scatter(wd, inner, r2_s, r2_r)
    for i in range(CHUNKS + 1):
        if i < CHUNKS:
            combine(i, r2_copies, r2_s, r2_r)
        if i:
            cs = pl.ds((i - 1) * CW, CW)
            out[:, cs] = (gath[my_rows, cs].astype(F32) + reduced(i - 1, r2_copies)).astype(BF)

    for cp in (*ag_copies.values(), *r2_copies.values()):
        cp.wait_send()
    for t in range(2):
        @pl.when(j < J - 1)
        def _():
            z_copy(b, t).wait_send()

        @pl.when(c == 0)
        def _():
            d_copy(b, t).wait_send()

    def drain(s, carry):
        slot = 2 * (j - 1 - s) + c
        for t in range(2):
            @pl.when(j < J - 1)
            def _():
                z_copy(slot, t).wait_send()

            d_copy(slot, t).wait_send()
        return carry

    lax.fori_loop(0, j, drain, 0)


def square_kernel(
    H, B,
    hid_h, q_h, k_h, v_h, gain_h, wo_h, wg_h, wu_h, wd_h,
    out,
    hid, q_in, k_in, v_in, gain, wo, wg, wu, wd, qb, kv, att, attx, hx, sb, rb, part, rs, gath, accg, accu, inner,
    i_sem, w_sem, a_s, a_r, z_s, z_r, d_s, d_r, x_s, x_r, at_s, at_r, o_s, o_r, ag_s, ag_r, r2_s, r2_r,
):
    h = lax.axis_index("head")
    b = lax.axis_index("blk")
    J = B // 2
    j = b // 2
    c = b % 2
    partner = b + 1 - 2 * c
    T, D = hid.shape
    R = T * H
    G = kv.shape[1]
    QW = qb.shape[1]
    ratio = QW // G // HEAD_DIM
    GW = QW // G
    FW = wg.shape[1]
    half = D // 2
    DW = D // 4
    grain = DW // sum(SUBS)
    subs = [(sum(SUBS[:i]) * grain, w * grain) for i, w in enumerate(SUBS)]

    ex, ey = h % 2, h // 2
    nx = h + 1 - 2 * ex
    ny = lax.rem(h + 2, H)
    dg = H - 1 - h
    pair = (nx, ny)
    across = (ny, nx)
    mine = (ex, ey)

    wcopies = []
    for s in range(2):
        src = wo_h.at[:, pl.ds(pl.multiple_of(s * half + mine[s] * DW, DW), DW)]
        wcopies.append((src, wo.at[s, pl.ds(0, QW)]))
    for i in range(CHUNKS):
        rows = pl.ds(i * (D // CHUNKS), D // CHUNKS)
        wcopies.append((wg_h.at[rows], wg.at[rows]))
        wcopies.append((wu_h.at[rows], wu.at[rows]))
    wcopies.append((wd_h, wd))
    wcopies = [pltpu.make_async_copy(s, d, w_sem.at[n]) for n, (s, d) in enumerate(wcopies)]

    staged = [
        pltpu.make_async_copy(src, dst, i_sem.at[n])
        for n, (src, dst) in enumerate(((k_h, k_in), (v_h, v_in), (q_h, q_in), (hid_h, hid), (gain_h, gain)))
    ]
    for cp in staged:
        cp.start()
    barrier = pltpu.get_barrier_semaphore()
    for d in range(1, H):
        pl.semaphore_signal(barrier, inc=1, device_id={"head": lax.rem(h + d, H)}, device_id_type=MESH)

    @pl.when(j > 0)
    def _():
        pl.semaphore_signal(barrier, inc=1, device_id={"blk": lax.rem(b + B - 2, B)}, device_id_type=MESH)

    @pl.when(j < J - 1)
    def _():
        pl.semaphore_signal(barrier, inc=1, device_id={"blk": lax.rem(b + 2, B)}, device_id_type=MESH)

    pl.semaphore_signal(barrier, inc=1, device_id={"blk": partner}, device_id_type=MESH)
    pl.semaphore_wait(barrier, H + jnp.minimum(j, 1) + jnp.minimum(J - 1 - j, 1))

    for cp in staged[:2]:
        cp.wait()

    def rows_of(p):
        return pl.ds(pl.multiple_of(p * T, T), T)

    my_rows = rows_of(h)

    pieces = []
    for g in range(G):
        pieces.append((k_in, G, g, kv.at[b, g, 0, my_rows, :]))
        pieces.append((v_in, G, g, kv.at[b, g, 1, my_rows, :]))
    pieces.append((q_in, 1, 0, qb.at[my_rows, :]))

    def piece_cols(p, per, n, dst):
        w = dst.shape[1]
        return pl.ds(pl.multiple_of((p * per + n) * w, w), w)

    a_copies = []
    for t, (src, per, n, dst) in enumerate(pieces):
        if src is q_in:
            staged[2].wait()
        cps = []
        for d, p in enumerate((dg, nx, ny)):
            cp = remote(src.at[:, piece_cols(p, per, n, dst)], dst, a_s.at[d, t], a_r.at[d, t], "head", p)
            cp.start()
            cps.append(cp)
        a_copies.append(cps)

    x_copies = []
    for s in range(2):
        cs = pl.ds(pl.multiple_of(s * half + (1 - mine[s]) * DW, DW), DW)
        x_copies.append(remote(hid.at[:, cs], hx.at[s], x_s.at[s], x_r.at[s], "head", pair[s]))
    core_cols = pl.ds(pl.multiple_of(c * (DW // 2), DW // 2), DW // 2)
    for s in range(2):
        cs = pl.ds(pl.multiple_of(s * half + (1 - mine[s]) * DW + c * (DW // 2), DW // 2), DW // 2)
        x_copies.append(remote(
            wo_h.at[:, cs], wo.at[s, pl.ds(QW, QW), core_cols],
            x_s.at[2 + s], x_r.at[2 + s], "head", pair[s],
        ))
    staged[3].wait()
    for cp in x_copies:
        cp.start()
    share = []
    for s in range(2):
        ref = wo.at[s, pl.ds(QW, QW), core_cols]
        share.append(remote(ref, ref, x_s.at[4 + s], x_r.at[4 + s], "blk", partner))

    for t, (src, per, n, dst) in enumerate(pieces):
        dst[...] = src[:, piece_cols(h, per, n, dst)]

    def wait_in(t):
        for cp in a_copies[t]:
            cp.wait_recv()

    def z_copy(slot, g, t):
        ref = kv.at[slot, g, t]
        return remote(ref, ref, z_s.at[slot, g, t], z_r.at[slot, g, t], "blk", lax.rem(b + 2, B))

    def d_copy(slot, g, t):
        ref = kv.at[slot, g, t]
        return remote(ref, ref, d_s.at[slot, g, t], d_r.at[slot, g, t], "blk", partner)

    own = [(g, t) for g in range(G) for t in range(2)]
    for n, (g, t) in enumerate(own):
        wait_in(n)

        @pl.when((j < J - 1) & ((j == 0) | (n < len(own) - 1)))
        def _():
            z_copy(b, g, t).start()

        @pl.when(c == 0)
        def _():
            d_copy(b, g, t).start()

    def pass_on(slot, g, t):
        z_copy(slot, g, t).wait_recv()

        @pl.when(j < J - 1)
        def _():
            z_copy(slot, g, t).start()

        d_copy(slot, g, t).start()

    def both(s):
        first = 2 * (j - 1 - s)
        return first + c, first + 1 - c

    def pass_on_first(g):
        @pl.when(j > 0)
        def _():
            for t in range(2):
                pass_on(both(0)[0], g, t)

    pass_on_first(0)

    @pl.when((j > 0) & (j < J - 1))
    def _():
        z_copy(b, *own[-1]).start()

    wait_in(len(own))
    for w in wcopies:
        w.start()

    factor = HEAD_DIM ** (-0.5) * LOG2E

    def absorb(g, slots, first):
        ones = jnp.ones((R, HEAD_DIM), BF)
        keys = jnp.concatenate([kv[slot, g, 0] for slot in slots], axis=0)
        values = jnp.concatenate(
            [jnp.concatenate([kv[slot, g, 1], ones], axis=1) for slot in slots], axis=0
        )
        for r in range(ratio):
            n = g * ratio + r
            tops = slice(n * HEAD_DIM, (n + 1) * HEAD_DIM)
            sums = slice(2 * n * HEAD_DIM, 2 * (n + 1) * HEAD_DIM)
            for q0 in range(0, R, QB):
                rows = slice(q0, q0 + QB)
                sc = lax.dot_general(
                    qb[rows, tops], keys,
                    (((1,), (1,)), ((), ())), preferred_element_type=F32,
                )
                tiles = [sc[:, t:t + HEAD_DIM] for t in range(0, len(slots) * R, HEAD_DIM)]
                if first:
                    qi = q0 + lax.broadcasted_iota(jnp.int32, tiles[0].shape, 0)
                    ki = lax.broadcasted_iota(jnp.int32, tiles[0].shape, 1)
                    for t in range(R // HEAD_DIM):
                        tiles[t] = jnp.where(ki + t * HEAD_DIM <= qi, tiles[t], -1e30)
                top = functools.reduce(jnp.maximum, tiles)
                top = jnp.broadcast_to(jnp.max(top, axis=1, keepdims=True), top.shape)
                if not first:
                    old = accu[rows, tops]
                    top = jnp.maximum(top, old)
                peak = top * factor
                e = jnp.concatenate([jnp.exp2(t * factor - peak).astype(BF) for t in tiles], axis=1)
                pv = jnp.dot(e, values, preferred_element_type=F32)
                if not first:
                    f = jnp.exp2(old * factor - peak)
                    pv = pv + accg[rows, sums] * jnp.concatenate([f, f], axis=1)
                accu[rows, tops] = top
                accg[rows, sums] = pv

    for g in range(G):
        @pl.when(c == 0)
        def _(g=g):
            absorb(g, (b,), True)

        @pl.when(c == 1)
        def _(g=g):
            for t in range(2):
                d_copy(b - 1, g, t).wait_recv()
            absorb(g, (b, b - 1), True)

    at_copies = []
    for g in range(G):
        def chain(s, carry, g=g):
            slot, other = both(s)

            @pl.when(s > 0)
            def _():
                for t in range(2):
                    pass_on(slot, g, t)

            for t in range(2):
                d_copy(other, g, t).wait_recv()
            absorb(g, (slot, other), False)
            return carry

        lax.fori_loop(0, j, chain, 0)
        if g + 1 < G:
            pass_on_first(g + 1)
        for r in range(ratio):
            n = g * ratio + r
            pv = accg[:, 2 * n * HEAD_DIM:2 * (n + 1) * HEAD_DIM]
            att[:, n * HEAD_DIM:(n + 1) * HEAD_DIM] = (pv[:, :HEAD_DIM] / pv[:, HEAD_DIM:]).astype(BF)
        cs = pl.ds(g * GW, GW)
        for s in range(2):
            cp = remote(att.at[:, cs], attx.at[s, :, cs], at_s.at[g, s], at_r.at[g, s], "head", pair[s])
            cp.start()
            at_copies.append(cp)

    accs = (accg, accu)
    for s in range(2):
        x_copies[2 + s].wait_recv()
        share[s].start()
    for s in range(2):
        wcopies[s].wait()
        for t in range(0, DW, tile_of(DW)):
            cs = slice(t, t + tile_of(DW))
            accs[s][:, cs] = jnp.dot(att[...], wo[s, :QW, cs], preferred_element_type=F32)
    for s in range(2):
        share[s].wait_recv()
    for cp in at_copies:
        cp.wait_recv()

    co = ({"h": nx, "x": h, "y": dg, "d": ny}, {"h": ny, "x": dg, "y": h, "d": nx})
    order = [(s, i) for i in range(len(subs)) for s in range(2)]
    o_copies = {}
    for s, i in order:
        cs = pl.ds(*subs[i])
        accs[s][:, cs] += jnp.dot(attx[s], wo[s, QW:, cs], preferred_element_type=F32)
        to = across[s]
        away = (to, co[s]["y" if s == 0 else "x"])
        for n, p in enumerate(away):
            sb[s, n * T:(n + 1) * T, cs] = accs[s][rows_of(p), cs].astype(BF)
        cp = remote(sb.at[s, :, cs], rb.at[s, :, cs], o_s.at[s, i], o_r.at[s, i], "head", to)
        cp.start()
        o_copies[s, i] = cp

    def cols_of(s, i, other):
        part_index = 1 - mine[s] if other else mine[s]
        at, w = subs[i]
        return pl.ds(pl.multiple_of(s * half + part_index * DW + at, grain), w)

    ag_copies = {}

    def spread(s, i, kind, rows, cs, to):
        ref = gath.at[rows, cs]
        cp = remote(ref, ref, ag_s.at[s, i, kind], ag_r.at[s, i, kind], "head", to)
        cp.start()
        ag_copies[s, i, kind] = cp

    def spread_own(s, i):
        cs = cols_of(s, i, False)
        for n, to in enumerate((nx, ny)):
            spread(s, i, 2 * n, my_rows, cs, to)
            spread(s, i, 2 * n + 1, rows_of(co[s]["h"]), cs, to)

    def relay(s, i):
        ag_copies[s, i, 0].wait_recv()
        spread(s, i, 4, rows_of(nx), cols_of(s, i, s == 0), ny)
        ag_copies[s, i, 3].wait_recv()
        spread(s, i, 5, rows_of(co[s]["y"]), cols_of(s, i, s == 1), nx)

    for s in range(2):
        x_copies[s].wait_recv()
    for k, (s, i) in enumerate(order):
        o_copies[s, i].wait_recv()
        cs = cols_of(s, i, False)
        lc = pl.ds(*subs[i])
        gath[my_rows, cs] = (
            hid[:, cs].astype(F32) + (accs[s][my_rows, lc] + rb[s, :T, lc].astype(F32))
        ).astype(BF)
        cr = rows_of(co[s]["h"])
        gath[cr, cs] = (
            hx[s, :, lc].astype(F32) + (accs[s][cr, lc] + rb[s, T:, lc].astype(F32))
        ).astype(BF)
        if k < LEAD:
            spread_own(s, i)

    staged[4].wait()
    for w in wcopies[2:-1]:
        w.wait()
    ft = tile_of(FW)
    square = jnp.zeros((R, 1), F32)
    for n in range(len(order) + LAG):
        if n < len(order):
            relay(*order[n])
            if n + LEAD < len(order):
                spread_own(*order[n + LEAD])
        if n < LAG:
            continue
        k = n - LAG
        s, i = order[k]
        for kind in (1, 2, 4, 5):
            ag_copies[s, i, kind].wait_recv()
        start, SW = subs[i]
        at = (s * half + start, s * half + DW + start)
        xs = []
        for a in at:
            x = gath[:, a:a + SW].astype(F32)
            square = square + jnp.sum(x * x, axis=1, keepdims=True)
            xs.append((x * gain[:, a:a + SW]).astype(BF))

        last = k == len(order) - 1
        if last:
            r = lax.rsqrt(square / D + 1e-5)
        for t in range(FW // ft):
            fs = slice(t * ft, (t + 1) * ft)
            ys = []
            for acc, w in ((accg, wg), (accu, wu)):
                y = jnp.dot(xs[0], w[at[0]:at[0] + SW, fs], preferred_element_type=F32)
                y = y + jnp.dot(xs[1], w[at[1]:at[1] + SW, fs], preferred_element_type=F32)
                if k:
                    y = y + acc[:, fs]
                if last:
                    ys.append(y * r)
                else:
                    acc[:, fs] = y
            if last:
                g, u = ys
                inner[:, fs] = (g / (1.0 + jnp.exp(-g)) * u).astype(BF)
    wcopies[-1].wait()

    unit = D // sum(WIDTHS)
    spans = [(sum(WIDTHS[:i]) * unit, w * unit) for i, w in enumerate(WIDTHS)]

    def halves(i):
        at, w = spans[i]
        return pl.ds(at, w // 2), pl.ds(at + w // 2, w // 2)

    copies = {}

    def send(i, sem, rows, place, cs, to):
        cp = remote(part.at[rows, cs], rs.at[place, :, cs], r2_s.at[sem, i], r2_r.at[sem, i], "head", to)
        cp.start()
        copies[sem, i] = cp

    for i, (at, w) in enumerate(spans):
        ct = tile_of(w)
        for t in range(w // ct):
            cs = slice(at + t * ct, at + (t + 1) * ct)
            part[:, cs] = jnp.dot(inner[...], wd[:, cs], preferred_element_type=F32).astype(BF)
        ha, hb = halves(i)
        send(i, 0, rows_of(dg), 1, ha, nx)
        send(i, 1, rows_of(dg), 1, hb, ny)
        send(i, 2, rows_of(nx), 0, ha, nx)
        send(i, 3, rows_of(ny), 0, hb, ny)
    for i in range(len(spans)):
        ha, hb = halves(i)
        for cs, sem, to in ((ha, 0, ny), (hb, 1, nx)):
            copies[sem, i].wait_recv()
            rows = rows_of(to)
            part[rows, cs] = (part[rows, cs].astype(F32) + rs[1, :, cs].astype(F32)).astype(BF)
            send(i, 4 + sem, rows, 2, cs, to)
    for i in range(len(spans)):
        cs = pl.ds(*spans[i])
        for sem in (2, 3, 4, 5):
            copies[sem, i].wait_recv()
        total = part[my_rows, cs].astype(F32)
        for place in (0, 2):
            total = total + rs[place, :, cs].astype(F32)
        out[:, cs] = (gath[my_rows, cs].astype(F32) + total).astype(BF)

    for cps in a_copies:
        for cp in cps:
            cp.wait_send()
    for cp in (*x_copies, *share, *at_copies, *o_copies.values(), *ag_copies.values(), *copies.values()):
        cp.wait_send()
    for g, t in own:
        @pl.when(j < J - 1)
        def _():
            z_copy(b, g, t).wait_send()

        @pl.when(c == 0)
        def _():
            d_copy(b, g, t).wait_send()

    def drain(s, carry):
        slot = 2 * (j - 1 - s) + c
        for g, t in own:
            @pl.when(j < J - 1)
            def _():
                z_copy(slot, g, t).wait_send()

            d_copy(slot, g, t).wait_send()
        return carry

    lax.fori_loop(0, j, drain, 0)


def square_call(H, B, hid, q, k, v, wo, gain, wg, wu, wd):
    T, D = hid.shape
    R = T * H
    QW = q.shape[1] // H
    G = k.shape[1] // H // HEAD_DIM
    FW = wg.shape[1]
    ratio = QW // HEAD_DIM // G
    AW = max(FW, D // 4, 2 * QW)
    vm = pl.BlockSpec(memory_space=pltpu.VMEM)
    hbm = pl.BlockSpec(memory_space=pl.ANY)
    dma = pltpu.SemaphoreType.DMA
    return pl.pallas_call(
        functools.partial(square_kernel, H, B),
        out_shape=pltpu.VMEM((T, D), BF),
        in_specs=[hbm] * 9,
        out_specs=vm,
        scratch_shapes=[
            pltpu.VMEM(hid.shape, BF),
            pltpu.VMEM(q.shape, BF),
            pltpu.VMEM(k.shape, BF),
            pltpu.VMEM(v.shape, BF),
            pltpu.VMEM((1, D), F32),
            pltpu.VMEM((2, 2 * QW, D // 4), BF),
            pltpu.VMEM(wg.shape, BF),
            pltpu.VMEM(wu.shape, BF),
            pltpu.VMEM(wd.shape, BF),
            pltpu.VMEM((R, QW), BF),
            pltpu.VMEM((B, G, 2, R, HEAD_DIM), BF),
            pltpu.VMEM((R, QW), BF),
            pltpu.VMEM((2, R, QW), BF),
            pltpu.VMEM((2, T, D // 4), BF),
            pltpu.VMEM((2, 2 * T, D // 4), BF),
            pltpu.VMEM((2, 2 * T, D // 4), BF),
            pltpu.VMEM((R, D), BF),
            pltpu.VMEM((3, T, D), BF),
            pltpu.VMEM((R, D), BF),
            pltpu.VMEM((R, AW), F32),
            pltpu.VMEM((R, AW), F32),
            pltpu.VMEM((R, FW), BF),
            dma((5,)),
            dma((3 + 2 * CHUNKS,)),
            dma((H - 1, 2 * G + 1)), dma((H - 1, 2 * G + 1)),
            dma((B, G, 2)), dma((B, G, 2)),
            dma((B, G, 2)), dma((B, G, 2)),
            dma((6,)), dma((6,)),
            dma((G, 2)), dma((G, 2)),
            dma((2, len(SUBS))), dma((2, len(SUBS))),
            dma((2, len(SUBS), 6)), dma((2, len(SUBS), 6)),
            dma((6, len(WIDTHS))), dma((6, len(WIDTHS))),
        ],
        compiler_params=pltpu.CompilerParams(
            collective_id=0, has_side_effects=True, vmem_limit_bytes=66_400_000
        ),
    )(hid, q, k, v, gain.reshape(1, -1), wo, wg, wu, wd)


def solution(mesh):
    H = mesh.shape["head"]
    B = mesh.shape["blk"]

    def local(hid, q, k, v, wo, gain, wg, wu, wd):
        if H == 4:
            return square_call(H, B, hid, q, k, v, wo, gain, wg, wu, wd)
        T, D = hid.shape
        R = T * H
        QW = q.shape[1] // H
        KW = k.shape[1] // H
        FW = wg.shape[1]
        vm = pl.BlockSpec(memory_space=pltpu.VMEM)
        hbm = pl.BlockSpec(memory_space=pl.ANY)
        dma = pltpu.SemaphoreType.DMA
        return pl.pallas_call(
            functools.partial(general_kernel, H, B),
            out_shape=jax.ShapeDtypeStruct((T, D), BF),
            in_specs=[vm] * 5 + [hbm] * 4,
            out_specs=vm,
            scratch_shapes=[
                pltpu.VMEM(wo.shape, BF),
                pltpu.VMEM(wg.shape, BF),
                pltpu.VMEM(wu.shape, BF),
                pltpu.VMEM(wd.shape, BF),
                pltpu.VMEM((R, QW), BF),
                pltpu.VMEM((B, 2, R, KW), BF),
                pltpu.VMEM((R, QW), BF),
                pltpu.VMEM((R, D), BF),
                pltpu.VMEM((H - 1, T, D), BF),
                pltpu.VMEM((R, D), BF),
                pltpu.VMEM((R, FW), F32),
                pltpu.VMEM((R, FW), F32),
                pltpu.VMEM((R, FW), BF),
                dma((2 + 2 * CHUNKS,)),
                dma((3,)),
                dma((H - 1, 3)), dma((H - 1, 3)),
                dma((B, 2)), dma((B, 2)),
                dma((B, 2)), dma((B, 2)),
                dma((max(H - 1, 6), CHUNKS)), dma((max(H - 1, 6), CHUNKS)),
                dma((max(H - 1, 6), CHUNKS)), dma((max(H - 1, 6), CHUNKS)),
                dma((max(H - 1, 6), CHUNKS)), dma((max(H - 1, 6), CHUNKS)),
            ],
            compiler_params=pltpu.CompilerParams(
                collective_id=0, has_side_effects=True, vmem_limit_bytes=67_043_328
            ),
        )(hid, q, k, v, gain.reshape(1, -1), wo, wg, wu, wd)

    rows = P(("blk", "head"), None)
    return jax.shard_map(
        local,
        mesh=mesh,
        in_specs=(rows, rows, rows, rows, P("head", None), P(), P(None, "head"), P(None, "head"), P("head", None)),
        out_specs=rows,
        check_vma=False,
    )
```
